16 devices in a mesh: tp: 2 (over z), ep: 8 (over y, x, core).
Axes of the slice: x: 2, y: 2, z: 2, core: 2. Of those that a mesh axis runs over, the one named last changes fastest.
Arguments:
- tokens: bfloat16 [6144, 1280], P(('ep', 'tp'))
- grad_y: bfloat16 [6144, 1280], P(('ep', 'tp'))
- expert_ids: int32 [6144, 6], P(('ep', 'tp'))
- gate_vals: float32 [6144, 6], P(('ep', 'tp'))
- slot_ids: int32 [6144, 6], P(('ep', 'tp'))
- shared_w1: bfloat16 [1280, 1792], P(None, 'tp')
- shared_w3: bfloat16 [1280, 1792], P(None, 'tp')
- shared_w2: bfloat16 [1792, 1280], P('tp')
- expert_w1: bfloat16 [64, 1280, 896], P('ep')
- expert_w3: bfloat16 [64, 1280, 896], P('ep')
- expert_w2: bfloat16 [64, 896, 1280], P('ep')
Outputs:
- output 1: bfloat16 [6144, 1280], P(('ep', 'tp'))
- output 2: bfloat16 [6144, 1280], P(('ep', 'tp'))
- output 3: bfloat16 [1280, 1792], P(None, 'tp')
- output 4: bfloat16 [1280, 1792], P(None, 'tp')
- output 5: bfloat16 [1792, 1280], P('tp')
- output 6: bfloat16 [64, 1280, 896], P('ep', 'tp')
- output 7: bfloat16 [64, 1280, 896], P('ep', 'tp')
- output 8: bfloat16 [64, 896, 1280], P('ep', 'tp')
All inputs are finite; a program needn't handle non-finite values.
Results may differ from the reference program's by a relative error of at most 0.00108.
Values are sent between devices in bfloat16 or wider.
A program may use at most 1 GiB of HBM per device.

```python
import jax
import jax.numpy as jnp
from jax import lax

MODEL_DIM = 1280
SHARED_FF = 1792
EXPERT_FF = 896
EXPERTS = 64
TOP_K = 6
SOURCES = 16
SOURCE_ROWS = 384
CAPACITY = 72


def gate_fn(proj_one, proj_three):
    return jax.nn.silu(proj_one) * proj_three


def routing_draw(route_key):
    noise_key, offset_key = jax.random.split(route_key)
    total_rows = SOURCES * SOURCE_ROWS
    offset = jax.random.randint(offset_key, (), 0, EXPERTS)
    expert_range = jnp.arange(EXPERTS, dtype=jnp.int32)
    favoured = ((expert_range - offset) % EXPERTS) < max(1, EXPERTS // 8)
    local_row = jnp.arange(total_rows, dtype=jnp.int32) % SOURCE_ROWS
    forced = (local_row[:, None] < CAPACITY) & (expert_range[None, :] == offset)
    race_weight = jnp.where(favoured, jnp.uint32(100), jnp.uint32(272))
    wait_time = (jax.random.bits(noise_key, (total_rows, EXPERTS), jnp.uint32) >> 16) * race_weight[None, :]
    scores = wait_time * jnp.uint32(EXPERTS) + expert_range.astype(jnp.uint32)[None, :] + jnp.uint32(EXPERTS)
    scores = jnp.where(forced, jnp.uint32(0), scores)
    expert_ids = jnp.argsort(scores, axis=-1)[:, :TOP_K].astype(jnp.int32)

    def source_slots(source_ids):
        onehot = (source_ids[:, None] == expert_range[None, :]).astype(jnp.int32)
        arrival = jnp.sum(jnp.cumsum(onehot, axis=0) * onehot, axis=1) - 1
        return jnp.where(arrival < CAPACITY, arrival, -1)

    slot_ids = lax.map(source_slots, expert_ids.reshape(SOURCES, SOURCE_ROWS * TOP_K))
    return expert_ids, slot_ids.reshape(total_rows, TOP_K).astype(jnp.int32)


def setup_inputs(seed: int = 0) -> dict:
    key_list = jax.random.split(jax.random.key(seed), 10)
    total_rows = SOURCES * SOURCE_ROWS
    tokens = jax.random.normal(key_list[0], (total_rows, MODEL_DIM), jnp.float32)
    grad_y = jax.random.normal(key_list[1], (total_rows, MODEL_DIM), jnp.float32)
    expert_ids, slot_ids = routing_draw(key_list[2])
    gate_vals = jax.random.uniform(key_list[3], (total_rows, TOP_K), jnp.float32, 0.4, 1.2) * TOP_K ** -0.5
    shared_w1 = jax.random.normal(key_list[4], (MODEL_DIM, SHARED_FF), jnp.float32) * MODEL_DIM ** -0.5
    shared_w3 = jax.random.normal(key_list[5], (MODEL_DIM, SHARED_FF), jnp.float32) * MODEL_DIM ** -0.5
    shared_w2 = jax.random.normal(key_list[6], (SHARED_FF, MODEL_DIM), jnp.float32) * SHARED_FF ** -0.5
    expert_w1 = jax.random.normal(key_list[7], (EXPERTS, MODEL_DIM, EXPERT_FF), jnp.float32) * MODEL_DIM ** -0.5
    expert_w3 = jax.random.normal(key_list[8], (EXPERTS, MODEL_DIM, EXPERT_FF), jnp.float32) * MODEL_DIM ** -0.5
    expert_w2 = jax.random.normal(key_list[9], (EXPERTS, EXPERT_FF, MODEL_DIM), jnp.float32) * EXPERT_FF ** -0.5
    return {
        "tokens": tokens.astype(jnp.bfloat16),
        "grad_y": grad_y.astype(jnp.bfloat16),
        "expert_ids": expert_ids,
        "gate_vals": gate_vals,
        "slot_ids": slot_ids,
        "shared_w1": shared_w1.astype(jnp.bfloat16),
        "shared_w3": shared_w3.astype(jnp.bfloat16),
        "shared_w2": shared_w2.astype(jnp.bfloat16),
        "expert_w1": expert_w1.astype(jnp.bfloat16),
        "expert_w3": expert_w3.astype(jnp.bfloat16),
        "expert_w2": expert_w2.astype(jnp.bfloat16),
    }


def swiglu_rows(in_rows, grad_rows, weight_one, weight_three, weight_two):
    proj_one = jnp.dot(in_rows, weight_one, preferred_element_type=jnp.float32)
    proj_three = jnp.dot(in_rows, weight_three, preferred_element_type=jnp.float32)
    gate_out, gate_vjp = jax.vjp(gate_fn, proj_one, proj_three)
    hidden = gate_out.astype(jnp.bfloat16)
    expert_out = jnp.dot(hidden, weight_two, preferred_element_type=jnp.float32)
    grad_hidden = jnp.dot(grad_rows, weight_two.T, preferred_element_type=jnp.float32).astype(jnp.bfloat16)
    grad_one, grad_three = gate_vjp(grad_hidden.astype(jnp.float32))
    grad_one = grad_one.astype(jnp.bfloat16)
    grad_three = grad_three.astype(jnp.bfloat16)
    grad_in = (jnp.dot(grad_one, weight_one.T, preferred_element_type=jnp.float32)
               + jnp.dot(grad_three, weight_three.T, preferred_element_type=jnp.float32))
    weight_grad_one = jnp.dot(in_rows.T, grad_one, preferred_element_type=jnp.float32)
    weight_grad_three = jnp.dot(in_rows.T, grad_three, preferred_element_type=jnp.float32)
    weight_grad_two = jnp.dot(hidden.T, grad_rows, preferred_element_type=jnp.float32)
    return expert_out, grad_in, weight_grad_one, weight_grad_three, weight_grad_two


def reference(tokens, grad_y, expert_ids, gate_vals, slot_ids, shared_w1, shared_w3, shared_w2,
              expert_w1, expert_w3, expert_w2):
    total_rows = SOURCES * SOURCE_ROWS
    copy_count = total_rows * TOP_K
    buffer_rows = EXPERTS * SOURCES * CAPACITY

    def shared_step(carry_in, block_xs):
        block_x, block_dy = block_xs
        expert_out, grad_in, grad_one, grad_three, grad_two = swiglu_rows(
            block_x, block_dy, shared_w1, shared_w3, shared_w2)
        carry_out = (carry_in[0] + grad_one, carry_in[1] + grad_three, carry_in[2] + grad_two)
        return carry_out, (expert_out, grad_in)

    shared_init = (jnp.zeros((MODEL_DIM, SHARED_FF), jnp.float32),
                   jnp.zeros((MODEL_DIM, SHARED_FF), jnp.float32),
                   jnp.zeros((SHARED_FF, MODEL_DIM), jnp.float32))
    shared_grads, shared_rows = lax.scan(
        shared_step, shared_init,
        (tokens.reshape(SOURCES, SOURCE_ROWS, MODEL_DIM), grad_y.reshape(SOURCES, SOURCE_ROWS, MODEL_DIM)))
    shared_out = shared_rows[0].reshape(total_rows, MODEL_DIM)
    shared_dx = shared_rows[1].reshape(total_rows, MODEL_DIM)

    source_of = jnp.arange(total_rows, dtype=jnp.int32) // SOURCE_ROWS
    flat_pos = jnp.where(slot_ids >= 0, (expert_ids * SOURCES + source_of[:, None]) * CAPACITY + slot_ids,
                         buffer_rows).reshape(-1)
    copy_of_row = jnp.full((buffer_rows,), copy_count, jnp.int32).at[flat_pos].set(
        jnp.arange(copy_count, dtype=jnp.int32), mode="drop")
    gates_flat = gate_vals.reshape(-1)

    def routed_step(carry_in, expert_xs):
        acc_y, acc_dx = carry_in
        weight_one, weight_three, weight_two, copy_rows = expert_xs
        token_rows = copy_rows // TOP_K
        row_gate = jnp.take(gates_flat, copy_rows, axis=0, mode="fill", fill_value=0)
        in_rows = jnp.take(tokens, token_rows, axis=0, mode="fill", fill_value=0)
        grad_rows = (row_gate[:, None] * jnp.take(grad_y, token_rows, axis=0, mode="fill", fill_value=0)
                     .astype(jnp.float32)).astype(jnp.bfloat16)
        expert_out, grad_in, grad_one, grad_three, grad_two = swiglu_rows(
            in_rows, grad_rows, weight_one, weight_three, weight_two)
        acc_y = acc_y.at[token_rows].add(
            row_gate[:, None] * expert_out.astype(jnp.bfloat16).astype(jnp.float32), mode="drop")
        acc_dx = acc_dx.at[token_rows].add(grad_in.astype(jnp.bfloat16).astype(jnp.float32), mode="drop")
        return (acc_y, acc_dx), (grad_one.astype(jnp.bfloat16), grad_three.astype(jnp.bfloat16),
                                 grad_two.astype(jnp.bfloat16))

    routed_init = (jnp.zeros((total_rows, MODEL_DIM), jnp.float32), jnp.zeros((total_rows, MODEL_DIM), jnp.float32))
    routed_acc, routed_grads = lax.scan(
        routed_step, routed_init,
        (expert_w1, expert_w3, expert_w2, copy_of_row.reshape(EXPERTS, SOURCES * CAPACITY)))
    out_y = (tokens.astype(jnp.float32) + shared_out + routed_acc[0]).astype(jnp.bfloat16)
    grad_tokens = (grad_y.astype(jnp.float32) + shared_dx + routed_acc[1]).astype(jnp.bfloat16)
    return (out_y, grad_tokens, shared_grads[0].astype(jnp.bfloat16), shared_grads[1].astype(jnp.bfloat16),
            shared_grads[2].astype(jnp.bfloat16), routed_grads[0], routed_grads[1], routed_grads[2])
```

```python
import functools

import jax
import jax.numpy as jnp
from jax import lax
from jax.experimental import pallas as pl
from jax.experimental.pallas import tpu as pltpu
from jax.sharding import PartitionSpec as P

F32 = jnp.float32
BF16 = jnp.bfloat16
SLICE = 128
VMEM_LIMIT = 64_000_000
NT = (((1,), (1,)), ((), ()))
TN = (((0,), (0,)), ((), ()))


def dot(a, b):
    return jnp.dot(a, b, preferred_element_type=F32)


def dot_nt(a, b):
    return lax.dot_general(a, b, NT, preferred_element_type=F32)


def dot_tn(a, b):
    return lax.dot_general(a, b, TN, preferred_element_type=F32)


def swiglu_parts(one, three, grad_hidden):
    sig = jax.nn.sigmoid(one)
    silu = one * sig
    dh = grad_hidden.astype(BF16).astype(F32)
    hidden = (silu * three).astype(BF16)
    da_one = (dh * three * (sig + silu * (1.0 - sig))).astype(BF16)
    da_three = (dh * silu).astype(BF16)
    return hidden, da_one, da_three


def params(axes):
    return pltpu.CompilerParams(dimension_semantics=("arbitrary",) * axes, vmem_limit_bytes=VMEM_LIMIT)


def dispatch_kernel(local, cap, top_k, ids, x_ref, dy_ref, meta_ref, xd_ref, qd_ref):
    tokens = x_ref.shape[-2]
    rows = local * cap
    meta = meta_ref[0, 0]
    base = (ids[1] * rows).astype(F32)
    row_ids = lax.broadcasted_iota(jnp.int32, (rows, tokens), 0).astype(F32) + base
    gates = jnp.zeros((rows, tokens), F32)
    for j in range(top_k):
        gates = jnp.where(meta[j][None, :] == row_ids, meta[top_k + j][None, :], gates)
    select = jnp.where(gates != 0.0, 1.0, 0.0).astype(BF16)
    row_gate = jnp.sum(gates, axis=1, keepdims=True)
    got_x = dot(select, x_ref[0, 0])
    for l in range(local):
        xd_ref[0, l] = got_x[l * cap:(l + 1) * cap].astype(BF16)
    got_dy = dot(select, dy_ref[0, 0]) * row_gate
    for l in range(local):
        qd_ref[0, l] = got_dy[l * cap:(l + 1) * cap].astype(BF16)


def dispatch(ids, x_all, dy_all, meta_all, local, cap, top_k, layers, first):
    groups, tps, tokens, dim = x_all.shape
    row_map = lambda y, s, ids: (s, (ids[0] + y + first) % tps, 0, 0)
    out = jax.ShapeDtypeStruct((layers, local, groups * cap, dim), BF16)
    out_spec = pl.BlockSpec((1, local, cap, dim), lambda y, s, ids: (y, 0, s, 0))
    return pl.pallas_call(
        functools.partial(dispatch_kernel, local, cap, top_k),
        grid_spec=pltpu.PrefetchScalarGridSpec(
            num_scalar_prefetch=1, grid=(layers, groups),
            in_specs=[pl.BlockSpec((1, 1, tokens, dim), row_map), pl.BlockSpec((1, 1, tokens, dim), row_map),
                      pl.BlockSpec((1, 1, 2 * top_k, tokens), row_map)],
            out_specs=[out_spec, out_spec]),
        out_shape=[out, out], compiler_params=params(2), name=f"dispatch{first}",
        cost_estimate=pl.CostEstimate(flops=layers * groups * local * cap * tokens * dim * 4,
                                      bytes_accessed=layers * groups * (tokens + local * cap) * dim * 4,
                                      transcendentals=0),
    )(ids, x_all, dy_all, meta_all)


def own_kernel(cap, x_ref, q_ref, w1_ref, w3_ref, w2_ref, o_ref, dr_ref, h_ref, da1_ref, da3_ref):
    rows = x_ref.shape[-2]
    groups = rows // cap
    half = rows // 2
    per = groups // 2
    for part in range(2):
        span = slice(part * half, (part + 1) * half)
        x = x_ref[0, 0, span]
        hidden, da_one, da_three = swiglu_parts(dot(x, w1_ref[0]), dot(x, w3_ref[0]),
                                                dot_nt(q_ref[0, 0, span], w2_ref[0]))
        h_ref[0, span] = hidden
        da1_ref[0, span] = da_one
        da3_ref[0, span] = da_three
        out = dot(hidden, w2_ref[0])
        grad = dot_nt(da_one, w1_ref[0]) + dot_nt(da_three, w3_ref[0])
        for s in range(per):
            o_ref[part * per + s] = out[s * cap:(s + 1) * cap].astype(BF16)
            dr_ref[part * per + s] = grad[s * cap:(s + 1) * cap].astype(BF16)


def own_experts(xd, qd, w1, w3, w2, cap):
    _, local, rows, dim = xd.shape
    ff = w1.shape[-1]
    groups = rows // cap
    row_spec = pl.BlockSpec((1, 1, rows, dim), lambda l: (0, l, 0, 0))
    back = jax.ShapeDtypeStruct((groups, local * cap, dim), BF16)
    back_spec = pl.BlockSpec((groups, cap, dim), lambda l: (0, l, 0))
    hid = jax.ShapeDtypeStruct((local, rows, ff), BF16)
    hid_spec = pl.BlockSpec((1, rows, ff), lambda l: (l, 0, 0))
    wide = pl.BlockSpec((1, dim, ff), lambda l: (l, 0, 0))
    tall = pl.BlockSpec((1, ff, dim), lambda l: (l, 0, 0))
    return pl.pallas_call(
        functools.partial(own_kernel, cap), grid=(local,),
        in_specs=[row_spec, row_spec, wide, wide, tall],
        out_specs=[back_spec, back_spec, hid_spec, hid_spec, hid_spec],
        out_shape=[back, back, hid, hid, hid], compiler_params=params(1), name="own",
        cost_estimate=pl.CostEstimate(flops=12 * local * rows * dim * ff,
                                      bytes_accessed=local * (8 * rows * dim + 6 * rows * ff + 6 * dim * ff),
                                      transcendentals=local * rows * ff),
    )(xd, qd, w1, w3, w2)


def grads_kernel(parts, ids, x_ref, q_ref, xp_ref, qp_ref, h_ref, da1_ref, da3_ref, w1_ref, w3_ref, w2_ref,
                 g1_ref, g3_ref, g2_ref, hid, da_one, da_three, tall):
    rows = x_ref.shape[-2]
    half = rows // 2
    hid[:rows] = h_ref[0]
    da_one[:rows] = da1_ref[0]
    da_three[:rows] = da3_ref[0]
    for part in range(2):
        span = slice(part * half, (part + 1) * half)
        dest = slice(rows + part * half, rows + (part + 1) * half)
        x = xp_ref[0, 0, span]
        hidden, one, three = swiglu_parts(dot(x, w1_ref[0]), dot(x, w3_ref[0]),
                                          dot_nt(qp_ref[0, 0, span], w2_ref[0]))
        hid[dest] = hidden
        da_one[dest] = one
        da_three[dest] = three
    part = ids[0]
    width = g1_ref.shape[1]
    columns = pl.ds(pl.multiple_of(part * width, 128), width)
    own_x = x_ref[0, 0, :, columns]
    far_x = xp_ref[0, 0, :, columns]
    g1_ref[0] = (dot_tn(own_x, da_one[:rows]) + dot_tn(far_x, da_one[rows:])).astype(BF16)
    g3_ref[0] = (dot_tn(own_x, da_three[:rows]) + dot_tn(far_x, da_three[rows:])).astype(BF16)
    height = g2_ref.shape[1]
    ff = hid.shape[1]
    reach = tall.shape[0]
    chunk = pl.ds(pl.multiple_of(part * (ff - reach), 128), reach)
    tall[...] = dot_tn(hid[:rows, chunk], q_ref[0, 0]) + dot_tn(hid[rows:, chunk], qp_ref[0, 0])
    skip = pl.multiple_of(part * (height - (ff - reach)), 8)
    g2_ref[0] = tall[pl.ds(skip, height)].astype(BF16)


def expert_grads(ids, xd, qd, xp, qp, h, da1, da3, w1, w3, w2, parts):
    _, local, rows, dim = xd.shape
    ff = w1.shape[-1]
    row_spec = pl.BlockSpec((1, 1, rows, dim), lambda l, ids: (0, l, 0, 0))
    hid_spec = pl.BlockSpec((1, rows, ff), lambda l, ids: (l, 0, 0))
    wide = pl.BlockSpec((1, dim, ff), lambda l, ids: (l, 0, 0))
    tall = pl.BlockSpec((1, ff, dim), lambda l, ids: (l, 0, 0))
    g1 = jax.ShapeDtypeStruct((local, dim // parts, ff), BF16)
    g2 = jax.ShapeDtypeStruct((local, ff // parts, dim), BF16)
    g1_spec = pl.BlockSpec((1, dim // parts, ff), lambda l, ids: (l, 0, 0))
    g2_spec = pl.BlockSpec((1, ff // parts, dim), lambda l, ids: (l, 0, 0))
    reach = -(-(ff // parts) // 128) * 128
    return pl.pallas_call(
        functools.partial(grads_kernel, parts),
        grid_spec=pltpu.PrefetchScalarGridSpec(
            num_scalar_prefetch=1, grid=(local,),
            in_specs=[row_spec, row_spec, row_spec, row_spec, hid_spec, hid_spec, hid_spec, wide, wide, tall],
            out_specs=[g1_spec, g1_spec, g2_spec],
            scratch_shapes=[pltpu.VMEM((2 * rows, ff), BF16)] * 3 + [pltpu.VMEM((reach, dim), F32)]),
        out_shape=[g1, g1, g2], compiler_params=params(1), name="grads",
        cost_estimate=pl.CostEstimate(flops=12 * local * rows * dim * ff,
                                      bytes_accessed=local * (8 * rows * dim + 6 * rows * ff + 9 * dim * ff),
                                      transcendentals=local * rows * ff),
    )(ids, xd, qd, xp, qp, h, da1, da3, w1, w3, w2)


def shared_kernel(ids, x_ref, dy_ref, wa_ref, w2_ref, h_ref, da_ref, ga_ref, g2_ref, acc_a, acc_2):
    layer, source = pl.program_id(0), pl.program_id(1)

    @pl.when((layer == 0) & (source == 0))
    def _():
        acc_a[...] = jnp.zeros_like(acc_a)
        acc_2[...] = jnp.zeros_like(acc_2)

    x, dy = x_ref[0, 0], dy_ref[0, 0]
    proj = dot(x, wa_ref[...])
    dh = dot_nt(dy, w2_ref[...])
    for half in range(2):
        one = proj[:, 2 * half * SLICE:(2 * half + 1) * SLICE]
        three = proj[:, (2 * half + 1) * SLICE:(2 * half + 2) * SLICE]
        hidden, da_one, da_three = swiglu_parts(one, three, dh[:, half * SLICE:(half + 1) * SLICE])
        h_ref[0, :, half * SLICE:(half + 1) * SLICE] = hidden
        da_ref[0, :, 2 * half * SLICE:(2 * half + 1) * SLICE] = da_one
        da_ref[0, :, (2 * half + 1) * SLICE:(2 * half + 2) * SLICE] = da_three
    acc_a[...] += dot_tn(x, da_ref[0, :, :2 * SLICE])
    acc_2[...] += dot_tn(h_ref[0, :, :SLICE], dy)

    @pl.when((layer == pl.num_programs(0) - 1) & (source == pl.num_programs(1) - 1))
    def _():
        ga_ref[...] = acc_a[...].astype(BF16)
        g2_ref[...] = acc_2[...].astype(BF16)


def shared_expert(ids, x_all, dy_all, wa, w2):
    groups, tps, tokens, dim = x_all.shape
    row_map = lambda y, s, ids: (s, (ids[0] + y) % tps, 0, 0)
    own_map = lambda y, s, ids: (jnp.where(y == 0, s, groups), 0, 0)
    fixed = lambda y, s, ids: (0, 0)
    return pl.pallas_call(
        shared_kernel,
        grid_spec=pltpu.PrefetchScalarGridSpec(
            num_scalar_prefetch=1, grid=(tps, groups),
            in_specs=[pl.BlockSpec((1, 1, tokens, dim), row_map), pl.BlockSpec((1, 1, tokens, dim), row_map),
                      pl.BlockSpec(wa.shape, fixed), pl.BlockSpec(w2.shape, fixed)],
            out_specs=[pl.BlockSpec((1, tokens, 2 * SLICE), own_map), pl.BlockSpec((1, tokens, 4 * SLICE), own_map),
                       pl.BlockSpec((dim, 2 * SLICE), fixed), pl.BlockSpec((SLICE, dim), fixed)],
            scratch_shapes=[pltpu.VMEM((dim, 2 * SLICE), F32), pltpu.VMEM((SLICE, dim), F32)]),
        out_shape=[jax.ShapeDtypeStruct((groups + 1, tokens, 2 * SLICE), BF16),
                   jax.ShapeDtypeStruct((groups + 1, tokens, 4 * SLICE), BF16),
                   jax.ShapeDtypeStruct((dim, 2 * SLICE), BF16), jax.ShapeDtypeStruct((SLICE, dim), BF16)],
        compiler_params=params(2), name="shared",
        cost_estimate=pl.CostEstimate(flops=18 * groups * tps * tokens * dim * SLICE,
                                      bytes_accessed=4 * groups * tps * tokens * dim, transcendentals=0),
    )(ids, x_all, dy_all, wa, w2)


def combine_kernel(local, cap, top_k, ids, meta_ref, o_ref, dr_ref, h_ref, da_ref, wa_ref, w2_ref, y_ref, dx_ref):
    tokens = h_ref.shape[-2]
    rows = local * cap
    meta = meta_ref[0]
    base = (ids[1] * rows).astype(F32)
    row_ids = lax.broadcasted_iota(jnp.int32, (tokens, rows), 1).astype(F32) + base
    gates = jnp.zeros((tokens, rows), F32)
    for j in range(top_k):
        gates = jnp.where(meta[:, j:j + 1] == row_ids, meta[:, top_k + j:top_k + j + 1], gates)
    high = gates.astype(BF16)
    rest = gates - high.astype(F32)
    mid = rest.astype(BF16)
    low = (rest - mid.astype(F32)).astype(BF16)
    out = o_ref[0]
    y_ref[0] = dot(high, out) + dot(mid, out) + dot(low, out) + dot(h_ref[0], w2_ref[...])
    select = jnp.where(gates != 0.0, 1.0, 0.0).astype(BF16)
    dx_ref[0] = dot(select, dr_ref[0]) + dot_nt(da_ref[0], wa_ref[...])


def combine(ids, meta_own, o, dr, h, da, wa, w2, local, cap, top_k):
    groups, rows, dim = o.shape
    tokens = h.shape[1]
    by_source = lambda s, ids: (s, 0, 0)
    fixed = lambda s, ids: (0, 0)
    out = jax.ShapeDtypeStruct((groups, tokens, dim), F32)
    out_spec = pl.BlockSpec((1, tokens, dim), by_source)
    return pl.pallas_call(
        functools.partial(combine_kernel, local, cap, top_k),
        grid_spec=pltpu.PrefetchScalarGridSpec(
            num_scalar_prefetch=1, grid=(groups,),
            in_specs=[pl.BlockSpec((1, tokens, 2 * top_k), by_source), pl.BlockSpec((1, rows, dim), by_source),
                      pl.BlockSpec((1, rows, dim), by_source), pl.BlockSpec((1, tokens, 2 * SLICE), by_source),
                      pl.BlockSpec((1, tokens, 4 * SLICE), by_source), pl.BlockSpec(wa.shape, fixed),
                      pl.BlockSpec(w2.shape, fixed)],
            out_specs=[out_spec, out_spec]),
        out_shape=[out, out], compiler_params=params(1), name="combine",
        cost_estimate=pl.CostEstimate(flops=8 * groups * tokens * rows * dim,
                                      bytes_accessed=groups * (4 * rows + 8 * tokens) * dim, transcendentals=0),
    )(ids, meta_own, o, dr, h, da, wa, w2)


def solution(mesh):
    ep_size, tp_size = mesh.shape["ep"], mesh.shape["tp"]
    row_spec = P(("ep", "tp"), None)
    expert_spec = P("ep", None, None)
    expert_grad_spec = P("ep", "tp", None)
    swap = [(0, 1), (1, 0)]

    def device_fn(tokens, grad_y, expert_ids, gate_vals, slot_ids,
                  shared_w1, shared_w3, shared_w2, expert_w1, expert_w3, expert_w2):
        rows_dev, dim = tokens.shape
        top_k = expert_ids.shape[1]
        local = expert_w1.shape[0]
        experts = local * ep_size
        cap = (2 * rows_dev * top_k + experts - 1) // experts
        tp_id, ep_id = lax.axis_index("tp"), lax.axis_index("ep")
        ids = jnp.stack([tp_id, ep_id]).astype(jnp.int32)

        pos = jnp.where(slot_ids >= 0, expert_ids * cap + slot_ids, -1).astype(F32)
        meta = jnp.concatenate([pos.T, gate_vals.T], axis=0)
        meta_all = lax.all_gather(meta, ("ep", "tp")).reshape(ep_size, tp_size, 2 * top_k, rows_dev)
        x_all = lax.all_gather(tokens, ("ep", "tp"), axis=0, tiled=True).reshape(ep_size, tp_size, rows_dev, dim)
        dy_all = lax.all_gather(grad_y, ("ep", "tp"), axis=0, tiled=True).reshape(ep_size, tp_size, rows_dev, dim)

        ff = shared_w1.shape[1]
        padded = ep_size * SLICE
        wide_pad = ((0, 0), (0, padded - ff))
        start = ep_id * SLICE
        w1s = lax.dynamic_slice(jnp.pad(shared_w1, wide_pad), (0, start), (dim, SLICE))
        w3s = lax.dynamic_slice(jnp.pad(shared_w3, wide_pad), (0, start), (dim, SLICE))
        w2s = lax.dynamic_slice(jnp.pad(shared_w2, ((0, padded - ff), (0, 0))), (start, 0), (SLICE, dim))
        wa_own = jnp.concatenate([w1s, w3s], axis=1)
        wa = jnp.concatenate([wa_own, lax.ppermute(wa_own, "tp", swap)], axis=1)
        w2a = jnp.concatenate([w2s, lax.ppermute(w2s, "tp", swap)], axis=0)

        xd, qd = dispatch(ids, x_all, dy_all, meta_all, local, cap, top_k, 1, 0)
        sh, sda, sga, sg2 = shared_expert(ids, x_all, dy_all, wa, w2a)
        o, dr, h, da1, da3 = own_experts(xd, qd, expert_w1, expert_w3, expert_w2, cap)
        meta_own = lax.dynamic_index_in_dim(meta_all, tp_id, axis=1, keepdims=False).transpose(0, 2, 1)
        y_part, dx_part = combine(ids, meta_own, o, dr, sh, sda, wa, w2a, local, cap, top_k)
        y_sum = lax.psum_scatter(y_part.reshape(-1, dim), "ep", scatter_dimension=0, tiled=True)
        dx_sum = lax.psum_scatter(dx_part.reshape(-1, dim), "ep", scatter_dimension=0, tiled=True)

        xp, qp = dispatch(ids, x_all, dy_all, meta_all, local, cap, top_k, 1, 1)
        g1, g3, g2 = expert_grads(ids, xd, qd, xp, qp, h, da1, da3, expert_w1, expert_w3, expert_w2, tp_size)

        sga_all = lax.all_gather(sga, "ep")
        sg2_all = lax.all_gather(sg2, "ep")
        sg1 = sga_all[:, :, :SLICE].transpose(1, 0, 2).reshape(dim, padded)[:, :ff]
        sg3 = sga_all[:, :, SLICE:].transpose(1, 0, 2).reshape(dim, padded)[:, :ff]
        sg2 = sg2_all.reshape(padded, dim)[:ff]
        out_y = (tokens.astype(F32) + y_sum).astype(BF16)
        grad_tokens = (grad_y.astype(F32) + dx_sum).astype(BF16)
        return out_y, grad_tokens, sg1, sg3, sg2, g1, g3, g2

    return jax.shard_map(
        device_fn, mesh=mesh,
        in_specs=(row_spec, row_spec, row_spec, row_spec, row_spec,
                  P(None, "tp"), P(None, "tp"), P("tp", None), expert_spec, expert_spec, expert_spec),
        out_specs=(row_spec, row_spec, P(None, "tp"), P(None, "tp"), P("tp", None),
                   expert_grad_spec, expert_grad_spec, expert_grad_spec),
        check_vma=False)
```

```python
import functools

import jax
import jax.numpy as jnp
from jax import lax
from jax.experimental import pallas as pl
from jax.experimental.pallas import tpu as pltpu
from jax.sharding import PartitionSpec as P


F32 = jnp.float32
BF16 = jnp.bfloat16
SLICE = 128
VMEM_LIMIT = 64_000_000
MESH = pl.DeviceIdType.MESH
NT = (((1,), (1,)), ((), ()))
TN = (((0,), (0,)), ((), ()))


def dot(a, b):
    return jnp.dot(a, b, preferred_element_type=F32)


def dot_nt(a, b):
    return lax.dot_general(a, b, NT, preferred_element_type=F32)


def dot_tn(a, b):
    return lax.dot_general(a, b, TN, preferred_element_type=F32)


def swiglu_parts(one, three, grad_hidden):
    sig = jax.nn.sigmoid(one)
    silu = one * sig
    dh = grad_hidden.astype(BF16).astype(F32)
    hidden = (silu * three).astype(BF16)
    da_one = (dh * three * (sig + silu * (1.0 - sig))).astype(BF16)
    da_three = (dh * silu).astype(BF16)
    return hidden, da_one, da_three


def params(axes):
    return pltpu.CompilerParams(dimension_semantics=("arbitrary",) * axes, vmem_limit_bytes=VMEM_LIMIT)


def gather_kernel(ep_size, x_ref, dy_ref, meta_ref, own_ref, near_x_ref, near_y_ref, other_own_ref, other_x_ref, other_y_ref,
                  far_own_ref, far_other_ref, meta_all_ref, mine, mine_meta, load_sem, store_sem, send_sem, recv_sem):
    me = lax.axis_index("ep")
    core_peer = me + 1 - 2 * (me % 2)
    x_peer = me + 2 - 4 * ((me // 2) % 2)
    y_peer = me + 4 - 8 * (me // 4)
    z_peer = 1 - lax.axis_index("tp")

    barrier = pltpu.get_barrier_semaphore()
    for k in range(1, ep_size):
        pl.semaphore_signal(barrier, inc=1, device_id={"ep": (me + k) % ep_size}, device_id_type=MESH)
    pl.semaphore_signal(barrier, inc=1, device_id={"tp": z_peer}, device_id_type=MESH)

    loads = [pltpu.make_async_copy(x_ref, mine.at[0], load_sem.at[0]),
             pltpu.make_async_copy(dy_ref, mine.at[1], load_sem.at[1]),
             pltpu.make_async_copy(meta_ref, mine_meta, load_sem.at[2])]
    for copy in loads:
        copy.start()
    for copy in loads:
        copy.wait()
    stores = [pltpu.make_async_copy(mine, own_ref.at[0], store_sem.at[0]),
              pltpu.make_async_copy(mine_meta, meta_all_ref.at[me], store_sem.at[1])]
    pl.semaphore_wait(barrier, ep_size)

    half = x_ref.shape[0] // 2
    low, high = pl.ds(0, half), pl.ds(half, half)
    started = []

    def send(device, src, dst):
        n = len(started)
        copy = pltpu.make_async_remote_copy(src_ref=src, dst_ref=dst, send_sem=send_sem.at[n], recv_sem=recv_sem.at[n],
                                            device_id=device, device_id_type=MESH)
        copy.start()
        started.append(copy)
        return copy

    to_x, to_y, to_core = {"ep": x_peer}, {"ep": y_peer}, {"ep": core_peer}
    from_x_low = send(to_x, mine.at[:, low], near_x_ref.at[0, :, low])
    from_y_high = send(to_y, mine.at[:, high], near_y_ref.at[0, :, high])
    from_z = send({"tp": z_peer}, mine, far_own_ref.at[0])
    from_x_high = send(to_x, mine.at[:, high], near_x_ref.at[0, :, high])
    from_y_low = send(to_y, mine.at[:, low], near_y_ref.at[0, :, low])
    waiting = [send({"ep": (me + k) % ep_size}, mine_meta, meta_all_ref.at[me]) for k in range(1, ep_size)]
    waiting.append(send(to_core, mine, other_own_ref.at[0]))
    for copy in stores:
        copy.start()
    from_x_low.wait_recv()
    corner_low = send(to_y, near_x_ref.at[0, :, low], near_y_ref.at[1, :, low])
    waiting.append(send(to_core, near_x_ref.at[0, :, low], other_x_ref.at[0, :, low]))
    from_y_high.wait_recv()
    corner_high = send(to_x, near_y_ref.at[0, :, high], near_y_ref.at[1, :, high])
    waiting.append(send(to_core, near_y_ref.at[0, :, high], other_y_ref.at[0, :, high]))
    from_x_high.wait_recv()
    waiting.append(send(to_core, near_x_ref.at[0, :, high], other_x_ref.at[0, :, high]))
    from_y_low.wait_recv()
    waiting.append(send(to_core, near_y_ref.at[0, :, low], other_y_ref.at[0, :, low]))
    from_z.wait_recv()
    waiting.append(send(to_core, far_own_ref.at[0], far_other_ref.at[0]))
    corner_low.wait_recv()
    waiting.append(send(to_core, near_y_ref.at[1, :, low], other_y_ref.at[1, :, low]))
    corner_high.wait_recv()
    waiting.append(send(to_core, near_y_ref.at[1, :, high], other_y_ref.at[1, :, high]))
    for copy in waiting:
        copy.wait_recv()
    for copy in started:
        copy.wait_send()
    for copy in stores:
        copy.wait()


def gather_layer(tokens, grad_y, meta, ep_size):
    rows, dim = tokens.shape
    one = jax.ShapeDtypeStruct((1, 2, rows, dim), tokens.dtype)
    two = jax.ShapeDtypeStruct((2, 2, rows, dim), tokens.dtype)
    anywhere = pl.BlockSpec(memory_space=pl.ANY)
    copies = 5 + (ep_size - 1) + 1 + 2 + 7
    return pl.pallas_call(
        functools.partial(gather_kernel, ep_size),
        in_specs=[anywhere] * 3, out_specs=[anywhere] * 9,
        out_shape=[one, one, two, one, one, two, one, one, jax.ShapeDtypeStruct((ep_size,) + meta.shape, meta.dtype)],
        scratch_shapes=[pltpu.VMEM((2, rows, dim), tokens.dtype), pltpu.VMEM(meta.shape, meta.dtype),
                        pltpu.SemaphoreType.DMA((3,)), pltpu.SemaphoreType.DMA((2,)),
                        pltpu.SemaphoreType.DMA((copies,)), pltpu.SemaphoreType.DMA((copies,))],
        compiler_params=pltpu.CompilerParams(collective_id=0, has_side_effects=True), name="gather",
        cost_estimate=pl.CostEstimate(flops=60_000_000_000, bytes_accessed=ep_size * rows * dim * 8, transcendentals=0),
    )(tokens, grad_y, meta)


def ep_of(source, ids):
    core = jnp.where(source < 4, ids[1] % 2, 1 - ids[1] % 2)
    return 2 * jnp.bitwise_xor(ids[1] // 2, source % 4) + core


def stream(refs, per_step, buffer, sem):
    blocks = [(ref, i) for ref in refs for i in range(ref.shape[0])]
    step = pl.program_id(0)
    steps = len(blocks) // per_step

    def copies(k):
        return [pltpu.make_async_copy(ref.at[i], buffer.at[k % 2, n], sem.at[k % 2, n])
                for n, (ref, i) in enumerate(blocks[k * per_step:(k + 1) * per_step])]

    @pl.when(step == 0)
    def _():
        for copy in copies(0):
            copy.start()

    for k in range(steps):
        @pl.when(step == k)
        def _():
            if k + 1 < steps:
                for copy in copies(k + 1):
                    copy.start()
            for copy in copies(k):
                copy.wait()

    return step % 2


def dispatch_kernel(local, cap, top_k, ids, *refs):
    *blocks, meta_ref, xd_ref, qd_ref, buffer, sem = refs
    slot = stream(blocks, 1, buffer, sem)
    tokens = buffer.shape[-2]
    rows = local * cap
    meta = meta_ref[0]
    base = (ids[1] * rows).astype(F32)
    row_ids = lax.broadcasted_iota(jnp.int32, (rows, tokens), 0).astype(F32) + base
    gates = jnp.zeros((rows, tokens), F32)
    for j in range(top_k):
        gates = jnp.where(meta[j][None, :] == row_ids, meta[top_k + j][None, :], gates)
    select = jnp.where(gates != 0.0, 1.0, 0.0).astype(BF16)
    row_gate = jnp.sum(gates, axis=1, keepdims=True)
    got_x = dot(select, buffer[slot, 0, 0])
    for l in range(local):
        xd_ref[l] = got_x[l * cap:(l + 1) * cap].astype(BF16)
    got_dy = dot(select, buffer[slot, 0, 1]) * row_gate
    for l in range(local):
        qd_ref[l] = got_dy[l * cap:(l + 1) * cap].astype(BF16)


def dispatch(ids, blocks, meta_all, local, cap, top_k):
    _, _, tokens, dim = blocks[0].shape
    groups = sum(block.shape[0] for block in blocks)
    out = jax.ShapeDtypeStruct((local, groups * cap, dim), BF16)
    out_spec = pl.BlockSpec((local, cap, dim), lambda s, ids: (0, s, 0))
    return pl.pallas_call(
        functools.partial(dispatch_kernel, local, cap, top_k),
        grid_spec=pltpu.PrefetchScalarGridSpec(
            num_scalar_prefetch=1, grid=(groups,),
            in_specs=[pl.BlockSpec(memory_space=pl.ANY)] * len(blocks)
            + [pl.BlockSpec((1, 2 * top_k, tokens), lambda s, ids: (ep_of(s, ids), 0, 0))],
            out_specs=[out_spec, out_spec],
            scratch_shapes=[pltpu.VMEM((2, 1, 2, tokens, dim), BF16), pltpu.SemaphoreType.DMA((2, 1))]),
        out_shape=[out, out], compiler_params=params(1),
        cost_estimate=pl.CostEstimate(flops=4 * groups * local * cap * tokens * dim,
                                      bytes_accessed=groups * (tokens + local * cap) * dim * 4, transcendentals=0),
    )(ids, *blocks, meta_all)


def own_kernel(cap, x_ref, q_ref, w1_ref, w3_ref, w2_ref, o_ref, h_ref, da1_ref, da3_ref):
    rows = x_ref.shape[-2]
    half = rows // 2
    per = half // cap
    for part in range(2):
        span = slice(part * half, (part + 1) * half)
        x = x_ref[0, span]
        hidden, da_one, da_three = swiglu_parts(dot(x, w1_ref[0]), dot(x, w3_ref[0]), dot_nt(q_ref[0, span], w2_ref[0]))
        h_ref[0, span] = hidden
        da1_ref[0, span] = da_one
        da3_ref[0, span] = da_three
        out = dot(hidden, w2_ref[0])
        for s in range(per):
            o_ref[part * per + s] = out[s * cap:(s + 1) * cap].astype(BF16)


def own_experts(xd, qd, w1, w3, w2, cap):
    local, rows, dim = xd.shape
    ff = w1.shape[-1]
    groups = rows // cap
    by_expert = lambda l: (l, 0, 0)
    row_spec = pl.BlockSpec((1, rows, dim), by_expert)
    hid = jax.ShapeDtypeStruct((local, rows, ff), BF16)
    hid_spec = pl.BlockSpec((1, rows, ff), by_expert)
    wide, tall = pl.BlockSpec((1, dim, ff), by_expert), pl.BlockSpec((1, ff, dim), by_expert)
    return pl.pallas_call(
        functools.partial(own_kernel, cap), grid=(local,),
        in_specs=[row_spec, row_spec, wide, wide, tall],
        out_specs=[pl.BlockSpec((groups, cap, dim), lambda l: (0, l, 0)), hid_spec, hid_spec, hid_spec],
        out_shape=[jax.ShapeDtypeStruct((groups, local * cap, dim), BF16), hid, hid, hid],
        compiler_params=params(1), name="own",
        cost_estimate=pl.CostEstimate(flops=8 * local * rows * dim * ff,
                                      bytes_accessed=local * (6 * rows * dim + 6 * rows * ff + 6 * dim * ff),
                                      transcendentals=local * rows * ff),
    )(xd, qd, w1, w3, w2)


def back_kernel(cap, da1_ref, da3_ref, w1_ref, w3_ref, dr_ref):
    grad = dot_nt(da1_ref[0], w1_ref[0]) + dot_nt(da3_ref[0], w3_ref[0])
    for s in range(dr_ref.shape[0]):
        dr_ref[s] = grad[s * cap:(s + 1) * cap].astype(BF16)


def own_back(da1, da3, w1, w3, cap):
    local, rows, ff = da1.shape
    dim = w1.shape[1]
    groups = rows // cap
    by_expert = lambda l: (l, 0, 0)
    hid_spec, wide = pl.BlockSpec((1, rows, ff), by_expert), pl.BlockSpec((1, dim, ff), by_expert)
    return pl.pallas_call(
        functools.partial(back_kernel, cap), grid=(local,),
        in_specs=[hid_spec, hid_spec, wide, wide],
        out_specs=pl.BlockSpec((groups, cap, dim), lambda l: (0, l, 0)),
        out_shape=jax.ShapeDtypeStruct((groups, local * cap, dim), BF16),
        compiler_params=params(1), name="back",
        cost_estimate=pl.CostEstimate(flops=4 * local * rows * dim * ff,
                                      bytes_accessed=local * (2 * rows * dim + 4 * rows * ff + 4 * dim * ff),
                                      transcendentals=0),
    )(da1, da3, w1, w3)


def grads_kernel(ids, x_ref, q_ref, xp_ref, qp_ref, h_ref, da1_ref, da3_ref, w1_ref, w3_ref, w2_ref,
                 g1_ref, g3_ref, g2_ref, rows_x, rows_q, hid, da_one, da_three, tall):
    rows = x_ref.shape[-2]
    half = rows // 2
    part = ids[0]
    width = g1_ref.shape[1]
    columns = pl.ds(pl.multiple_of(part * width, 128), width)
    ff = w1_ref.shape[-1]
    reach = tall.shape[0]
    chunk = pl.ds(pl.multiple_of(part * (ff - reach), 128), reach)
    rows_x[:rows] = x_ref[0, :, columns]
    rows_x[rows:] = xp_ref[0, :, columns]
    rows_q[:rows] = q_ref[0]
    rows_q[rows:] = qp_ref[0]
    hid[:rows] = h_ref[0]
    da_one[:rows] = da1_ref[0]
    da_three[:rows] = da3_ref[0]
    for piece in range(2):
        span = slice(piece * half, (piece + 1) * half)
        dest = slice(rows + piece * half, rows + (piece + 1) * half)
        x = xp_ref[0, span]
        hidden, one, three = swiglu_parts(dot(x, w1_ref[0]), dot(x, w3_ref[0]), dot_nt(qp_ref[0, span], w2_ref[0]))
        hid[dest] = hidden
        da_one[dest] = one
        da_three[dest] = three
    g1_ref[0] = dot_tn(rows_x[...], da_one[...]).astype(BF16)
    g3_ref[0] = dot_tn(rows_x[...], da_three[...]).astype(BF16)
    height = g2_ref.shape[1]
    tall[...] = dot_tn(hid[:, chunk], rows_q[...])
    skip = pl.multiple_of(part * (height - (ff - reach)), 8)
    g2_ref[0] = tall[pl.ds(skip, height)].astype(BF16)


def expert_grads(ids, xd, qd, xp, qp, h, da1, da3, w1, w3, w2, parts):
    local, rows, dim = xd.shape
    ff = w1.shape[-1]
    by_expert = lambda l, ids: (l, 0, 0)
    row_spec, hid_spec = pl.BlockSpec((1, rows, dim), by_expert), pl.BlockSpec((1, rows, ff), by_expert)
    wide, tall = pl.BlockSpec((1, dim, ff), by_expert), pl.BlockSpec((1, ff, dim), by_expert)
    g1 = jax.ShapeDtypeStruct((local, dim // parts, ff), BF16)
    g2 = jax.ShapeDtypeStruct((local, ff // parts, dim), BF16)
    g1_spec, g2_spec = pl.BlockSpec((1, dim // parts, ff), by_expert), pl.BlockSpec((1, ff // parts, dim), by_expert)
    reach = -(-(ff // parts) // 128) * 128
    return pl.pallas_call(
        grads_kernel,
        grid_spec=pltpu.PrefetchScalarGridSpec(
            num_scalar_prefetch=1, grid=(local,),
            in_specs=[row_spec, row_spec, row_spec, row_spec, hid_spec, hid_spec, hid_spec, wide, wide, tall],
            out_specs=[g1_spec, g1_spec, g2_spec],
            scratch_shapes=[pltpu.VMEM((2 * rows, dim // parts), BF16), pltpu.VMEM((2 * rows, dim), BF16)]
            + [pltpu.VMEM((2 * rows, ff), BF16)] * 3 + [pltpu.VMEM((reach, dim), F32)]),
        out_shape=[g1, g1, g2], compiler_params=params(1), name="grads",
        cost_estimate=pl.CostEstimate(flops=12 * local * rows * dim * ff,
                                      bytes_accessed=local * (8 * rows * dim + 6 * rows * ff + 9 * dim * ff),
                                      transcendentals=local * rows * ff),
    )(ids, xd, qd, xp, qp, h, da1, da3, w1, w3, w2)


def shared_kernel(*refs):
    *blocks, wa_ref, w2_ref, h_ref, da_ref, g_ref, g_far_ref, buffer, sem = refs
    slot = stream(blocks, 2, buffer, sem)

    @pl.when(pl.program_id(0) == 0)
    def _():
        g_ref[...] = jnp.zeros_like(g_ref)
        g_far_ref[...] = jnp.zeros_like(g_far_ref)

    _, pair, _, tokens, dim = buffer.shape
    x = buffer[slot, :, 0].reshape(pair * tokens, dim)
    dy = buffer[slot, :, 1].reshape(pair * tokens, dim)
    proj = dot(x, wa_ref[...])
    dh = dot_nt(dy, w2_ref[...])
    for half, grad_ref in enumerate((g_ref, g_far_ref)):
        one = proj[:, 2 * half * SLICE:(2 * half + 1) * SLICE]
        three = proj[:, (2 * half + 1) * SLICE:(2 * half + 2) * SLICE]
        hidden, da_one, da_three = swiglu_parts(one, three, dh[:, half * SLICE:(half + 1) * SLICE])
        da = jnp.concatenate([da_one, da_three], axis=1)
        h_ref[:, :, half * SLICE:(half + 1) * SLICE] = hidden.reshape(pair, tokens, SLICE)
        da_ref[:, :, 2 * half * SLICE:2 * (half + 1) * SLICE] = da.reshape(pair, tokens, 2 * SLICE)
        grad_ref[:2 * SLICE] += dot_tn(da, x)
        grad_ref[2 * SLICE:] += dot_tn(hidden, dy)


def shared_expert(blocks, wa, w2):
    _, _, tokens, dim = blocks[0].shape
    groups = sum(block.shape[0] for block in blocks)
    by_pair, fixed = lambda s: (s, 0, 0), lambda s: (0, 0)
    grad = jax.ShapeDtypeStruct((3 * SLICE, dim), F32)
    return pl.pallas_call(
        shared_kernel, grid=(groups // 2,),
        in_specs=[pl.BlockSpec(memory_space=pl.ANY)] * len(blocks)
        + [pl.BlockSpec(wa.shape, fixed), pl.BlockSpec(w2.shape, fixed)],
        out_specs=[pl.BlockSpec((2, tokens, 2 * SLICE), by_pair), pl.BlockSpec((2, tokens, 4 * SLICE), by_pair),
                   pl.BlockSpec(grad.shape, fixed), pl.BlockSpec(grad.shape, fixed)],
        out_shape=[jax.ShapeDtypeStruct((groups, tokens, 2 * SLICE), BF16),
                   jax.ShapeDtypeStruct((groups, tokens, 4 * SLICE), BF16), grad, grad],
        scratch_shapes=[pltpu.VMEM((2, 2, 2, tokens, dim), BF16), pltpu.SemaphoreType.DMA((2, 2))],
        compiler_params=params(1), name="shared",
        cost_estimate=pl.CostEstimate(flops=18 * groups * tokens * dim * SLICE,
                                      bytes_accessed=4 * groups * tokens * dim, transcendentals=0),
    )(*blocks, wa, w2)


def gate_matrix(meta, ids, rows, top_k):
    tokens = meta.shape[0]
    base = (ids[1] * rows).astype(F32)
    row_ids = lax.broadcasted_iota(jnp.int32, (tokens, rows), 1).astype(F32) + base
    gates = jnp.zeros((tokens, rows), F32)
    for j in range(top_k):
        gates = jnp.where(meta[:, j:j + 1] == row_ids, meta[:, top_k + j:top_k + j + 1], gates)
    return gates


def combine_out_kernel(top_k, ids, meta_ref, o_ref, h_ref, w2_ref, y_ref):
    tokens = h_ref.shape[1]
    gates = gate_matrix(meta_ref[0], ids, o_ref.shape[1], top_k)
    high = gates.astype(BF16)
    rest = gates - high.astype(F32)
    mid = rest.astype(BF16)
    low = (rest - mid.astype(F32)).astype(BF16)
    sums = dot(jnp.concatenate([high, mid, low], axis=0), o_ref[0])
    y_ref[0] = sums[:tokens] + sums[tokens:2 * tokens] + sums[2 * tokens:] + dot(h_ref[0], w2_ref[...])


def combine_back_kernel(top_k, ids, meta_ref, dr_ref, da_ref, wa_ref, dx_ref):
    gates = gate_matrix(meta_ref[0], ids, dr_ref.shape[1], top_k)
    select = jnp.where(gates != 0.0, 1.0, 0.0).astype(BF16)
    dx_ref[0] = dot(select, dr_ref[0]) + dot_nt(da_ref[0], wa_ref[...])


def combine(kernel, ids, meta_own, returned, hidden, weight, top_k, passes):
    groups, rows, dim = returned.shape
    tokens, width = hidden.shape[1:]
    by_source = lambda s, ids: (s, 0, 0)
    by_ep = lambda s, ids: (ep_of(s, ids), 0, 0)
    return pl.pallas_call(
        functools.partial(kernel, top_k),
        grid_spec=pltpu.PrefetchScalarGridSpec(
            num_scalar_prefetch=1, grid=(groups,),
            in_specs=[pl.BlockSpec((1, tokens, 2 * top_k), by_ep), pl.BlockSpec((1, rows, dim), by_source),
                      pl.BlockSpec((1, tokens, width), by_source), pl.BlockSpec(weight.shape, lambda s, ids: (0, 0))],
            out_specs=pl.BlockSpec((1, tokens, dim), by_ep)),
        out_shape=jax.ShapeDtypeStruct((groups, tokens, dim), F32), compiler_params=params(1),
        cost_estimate=pl.CostEstimate(flops=2 * passes * groups * tokens * rows * dim,
                                      bytes_accessed=groups * (2 * rows + 4 * tokens) * dim, transcendentals=0),
    )(ids, meta_own, returned, hidden, weight)


def solution(mesh):
    ep_size, tp_size = mesh.shape["ep"], mesh.shape["tp"]
    row_spec = P(("ep", "tp"), None)
    expert_spec = P("ep", None, None)
    expert_grad_spec = P("ep", "tp", None)
    swap = [(0, 1), (1, 0)]
    cores = [(i, i ^ 1) for i in range(ep_size)]

    def device_fn(tokens, grad_y, expert_ids, gate_vals, slot_ids,
                  shared_w1, shared_w3, shared_w2, expert_w1, expert_w3, expert_w2):
        rows_dev, dim = tokens.shape
        top_k = expert_ids.shape[1]
        local = expert_w1.shape[0]
        experts = local * ep_size
        cap = (2 * rows_dev * top_k + experts - 1) // experts
        tp_id, ep_id = lax.axis_index("tp"), lax.axis_index("ep")
        ids = jnp.stack([tp_id, ep_id]).astype(jnp.int32)

        pos = jnp.where(slot_ids >= 0, expert_ids * cap + slot_ids, -1).astype(F32)
        meta = jnp.concatenate([pos.T, gate_vals.T], axis=0)
        *gathered, meta_all = gather_layer(tokens, grad_y, meta, ep_size)
        blocks, (far_own, far_other) = gathered[:6], gathered[6:]
        far_meta = lax.ppermute(meta_all, "tp", swap)
        far_x = lax.ppermute(blocks[1], "tp", swap)
        far_y = lax.ppermute(blocks[2], "tp", swap)
        cross_x = lax.ppermute(far_x, "ep", cores)
        cross_y = lax.ppermute(far_y, "ep", cores)

        ff = shared_w1.shape[1]
        padded = ep_size * SLICE
        wide_pad = ((0, 0), (0, padded - ff))
        start = ep_id * SLICE
        w1s = lax.dynamic_slice(jnp.pad(shared_w1, wide_pad), (0, start), (dim, SLICE))
        w3s = lax.dynamic_slice(jnp.pad(shared_w3, wide_pad), (0, start), (dim, SLICE))
        w2s = lax.dynamic_slice(jnp.pad(shared_w2, ((0, padded - ff), (0, 0))), (start, 0), (SLICE, dim))
        wa_own = jnp.concatenate([w1s, w3s], axis=1)
        wa = jnp.concatenate([wa_own, lax.ppermute(wa_own, "tp", swap)], axis=1)
        w2a = jnp.concatenate([w2s, lax.ppermute(w2s, "tp", swap)], axis=0)

        xd, qd = dispatch(ids, blocks, meta_all, local, cap, top_k)
        sh, sda, shared_grad, shared_far = shared_expert(blocks, wa, w2a)
        o, h, da1, da3 = own_experts(xd, qd, expert_w1, expert_w3, expert_w2, cap)
        meta_own = meta_all.transpose(0, 2, 1)
        y_part = combine(combine_out_kernel, ids, meta_own, o, sh, w2a, top_k, 3)
        y_sum = lax.psum_scatter(y_part.reshape(-1, dim), "ep", scatter_dimension=0, tiled=True)
        dr = own_back(da1, da3, expert_w1, expert_w3, cap)
        dx_part = combine(combine_back_kernel, ids, meta_own, dr, sda, wa, top_k, 1)
        dx_sum = lax.psum_scatter(dx_part.reshape(-1, dim), "ep", scatter_dimension=0, tiled=True)

        xp, qp = dispatch(ids, (far_own, far_x, far_y, far_other, cross_x, cross_y), far_meta, local, cap, top_k)
        g1, g3, g2 = expert_grads(ids, xd, qd, xp, qp, h, da1, da3, expert_w1, expert_w3, expert_w2, tp_size)

        shared_grad = shared_grad + lax.ppermute(shared_far, "tp", swap)
        shared_all = lax.all_gather(shared_grad.astype(BF16), "ep")
        sg1, sg3, sg2 = [shared_all[:, i * SLICE:(i + 1) * SLICE].reshape(padded, dim)[:ff] for i in range(3)]
        sg1, sg3 = sg1.T, sg3.T
        out_y = (tokens.astype(F32) + y_sum).astype(BF16)
        grad_tokens = (grad_y.astype(F32) + dx_sum).astype(BF16)
        return out_y, grad_tokens, sg1, sg3, sg2, g1, g3, g2

    return jax.shard_map(
        device_fn, mesh=mesh,
        in_specs=(row_spec, row_spec, row_spec, row_spec, row_spec,
                  P(None, "tp"), P(None, "tp"), P("tp", None), expert_spec, expert_spec, expert_spec),
        out_specs=(row_spec, row_spec, P(None, "tp"), P(None, "tp"), P("tp", None),
                   expert_grad_spec, expert_grad_spec, expert_grad_spec),
        check_vma=False)
```

```python
import functools

import jax
import jax.numpy as jnp
from jax import lax
from jax.experimental import pallas as pl
from jax.experimental.pallas import tpu as pltpu
from jax.sharding import PartitionSpec as P


F32 = jnp.float32
BF16 = jnp.bfloat16
SLICE = 128
VMEM_LIMIT = 64_000_000
MESH = pl.DeviceIdType.MESH
NT = (((1,), (1,)), ((), ()))
TN = (((0,), (0,)), ((), ()))


def dot(a, b):
    return jnp.dot(a, b, preferred_element_type=F32)


def dot_nt(a, b):
    return lax.dot_general(a, b, NT, preferred_element_type=F32)


def dot_tn(a, b):
    return lax.dot_general(a, b, TN, preferred_element_type=F32)


def swiglu_parts(one, three, grad_hidden):
    sig = jax.nn.sigmoid(one)
    silu = one * sig
    dh = grad_hidden.astype(BF16).astype(F32)
    hidden = (silu * three).astype(BF16)
    da_one = (dh * three * (sig + silu * (1.0 - sig))).astype(BF16)
    da_three = (dh * silu).astype(BF16)
    return hidden, da_one, da_three


def params(axes):
    return pltpu.CompilerParams(dimension_semantics=("arbitrary",) * axes, vmem_limit_bytes=VMEM_LIMIT)


def gather_kernel(ep_size, x_ref, dy_ref, meta_ref, near_x_ref, near_y_ref, other_own_ref, other_x_ref, other_y_ref,
                  far_own_ref, far_other_ref, meta_all_ref, dy_out_ref, mine, mine_dy, mine_meta,
                  load_sem, store_sem, send_sem, recv_sem):
    me = lax.axis_index("ep")
    core_peer = me + 1 - 2 * (me % 2)
    x_peer = me + 2 - 4 * ((me // 2) % 2)
    y_peer = me + 4 - 8 * (me // 4)
    z_peer = 1 - lax.axis_index("tp")

    barrier = pltpu.get_barrier_semaphore()
    for k in range(1, ep_size):
        pl.semaphore_signal(barrier, inc=1, device_id={"ep": (me + k) % ep_size}, device_id_type=MESH)
    pl.semaphore_signal(barrier, inc=1, device_id={"tp": z_peer}, device_id_type=MESH)

    loads = [pltpu.make_async_copy(x_ref, mine, load_sem.at[0]),
             pltpu.make_async_copy(meta_ref, mine_meta, load_sem.at[1]),
             pltpu.make_async_copy(dy_ref, mine_dy, load_sem.at[2])]
    for copy in loads:
        copy.start()
    for copy in loads:
        copy.wait()
    stores = [pltpu.make_async_copy(mine_dy, dy_out_ref, store_sem.at[0]),
              pltpu.make_async_copy(mine_meta, meta_all_ref.at[me], store_sem.at[1])]
    pl.semaphore_wait(barrier, ep_size)

    half = x_ref.shape[0] // 2
    low, high = pl.ds(0, half), pl.ds(half, half)
    started = []

    def send(device, src, dst):
        n = len(started)
        copy = pltpu.make_async_remote_copy(src_ref=src, dst_ref=dst, send_sem=send_sem.at[n], recv_sem=recv_sem.at[n],
                                            device_id=device, device_id_type=MESH)
        copy.start()
        started.append(copy)
        return copy

    to_x, to_y, to_core = {"ep": x_peer}, {"ep": y_peer}, {"ep": core_peer}
    from_x_low = send(to_x, mine.at[low], near_x_ref.at[0, low])
    from_y_high = send(to_y, mine.at[high], near_y_ref.at[0, high])
    from_z = send({"tp": z_peer}, mine, far_own_ref.at[0])
    from_x_high = send(to_x, mine.at[high], near_x_ref.at[0, high])
    from_y_low = send(to_y, mine.at[low], near_y_ref.at[0, low])
    waiting = [send({"ep": (me + k) % ep_size}, mine_meta, meta_all_ref.at[me]) for k in range(1, ep_size)]
    waiting.append(send(to_core, mine, other_own_ref.at[0]))
    for copy in stores:
        copy.start()
    from_x_low.wait_recv()
    corner_low = send(to_y, near_x_ref.at[0, low], near_y_ref.at[1, low])
    waiting.append(send(to_core, near_x_ref.at[0, low], other_x_ref.at[0, low]))
    from_y_high.wait_recv()
    corner_high = send(to_x, near_y_ref.at[0, high], near_y_ref.at[1, high])
    waiting.append(send(to_core, near_y_ref.at[0, high], other_y_ref.at[0, high]))
    from_x_high.wait_recv()
    waiting.append(send(to_core, near_x_ref.at[0, high], other_x_ref.at[0, high]))
    from_y_low.wait_recv()
    waiting.append(send(to_core, near_y_ref.at[0, low], other_y_ref.at[0, low]))
    from_z.wait_recv()
    waiting.append(send(to_core, far_own_ref.at[0], far_other_ref.at[0]))
    corner_low.wait_recv()
    waiting.append(send(to_core, near_y_ref.at[1, low], other_y_ref.at[1, low]))
    corner_high.wait_recv()
    waiting.append(send(to_core, near_y_ref.at[1, high], other_y_ref.at[1, high]))
    for copy in waiting:
        copy.wait_recv()
    for copy in started:
        copy.wait_send()
    for copy in stores:
        copy.wait()


def gather_layer(tokens, grad_y, meta, ep_size):
    rows, dim = tokens.shape
    one = jax.ShapeDtypeStruct((1, rows, dim), tokens.dtype)
    two = jax.ShapeDtypeStruct((2, rows, dim), tokens.dtype)
    anywhere = pl.BlockSpec(memory_space=pl.ANY)
    copies = 5 + (ep_size - 1) + 1 + 2 + 7
    return pl.pallas_call(
        functools.partial(gather_kernel, ep_size),
        in_specs=[anywhere] * 3, out_specs=[anywhere] * 9,
        out_shape=[one, two, one, one, two, one, one, jax.ShapeDtypeStruct((ep_size,) + meta.shape, meta.dtype),
                   jax.ShapeDtypeStruct(grad_y.shape, grad_y.dtype)],
        scratch_shapes=[pltpu.VMEM((rows, dim), tokens.dtype), pltpu.VMEM((rows, dim), grad_y.dtype),
                        pltpu.VMEM(meta.shape, meta.dtype), pltpu.SemaphoreType.DMA((3,)), pltpu.SemaphoreType.DMA((2,)),
                        pltpu.SemaphoreType.DMA((copies,)), pltpu.SemaphoreType.DMA((copies,))],
        compiler_params=pltpu.CompilerParams(collective_id=0, has_side_effects=True), name="gather",
        cost_estimate=pl.CostEstimate(flops=30_000_000_000, bytes_accessed=ep_size * rows * dim * 8, transcendentals=0),
    )(tokens, grad_y, meta)


def ep_of(source, ids):
    core = jnp.where(source < 4, ids[1] % 2, 1 - ids[1] % 2)
    return 2 * jnp.bitwise_xor(ids[1] // 2, source % 4) + core


def stream(refs, per_step, buffer, sem):
    blocks = [(ref, i) for ref in refs for i in range(ref.shape[0])]
    step = pl.program_id(0)
    steps = len(blocks) // per_step

    def copies(k):
        return [pltpu.make_async_copy(ref.at[i], buffer.at[k % 2, n], sem.at[k % 2, n])
                for n, (ref, i) in enumerate(blocks[k * per_step:(k + 1) * per_step])]

    @pl.when(step == 0)
    def _():
        for copy in copies(0):
            copy.start()

    for k in range(steps):
        @pl.when(step == k)
        def _():
            if k + 1 < steps:
                for copy in copies(k + 1):
                    copy.start()
            for copy in copies(k):
                copy.wait()

    return step % 2


def lay_rows(local, cap, got, out_ref):
    for l in range(local):
        out_ref[l] = got[l * cap:(l + 1) * cap].astype(BF16)


def gate_rows(meta, ids, rows, top_k):
    tokens = meta.shape[1]
    base = (ids[1] * rows).astype(F32)
    row_ids = lax.broadcasted_iota(jnp.int32, (rows, tokens), 0).astype(F32) + base
    gates = jnp.zeros((rows, tokens), F32)
    for j in range(top_k):
        gates = jnp.where(meta[j][None, :] == row_ids, meta[top_k + j][None, :], gates)
    return gates, jnp.where(gates != 0.0, 1.0, 0.0).astype(BF16)


def dispatch_x_kernel(local, cap, top_k, ids, *refs):
    *blocks, meta_ref, xd_ref, select_ref, gate_ref, buffer, sem = refs
    slot = stream(blocks, 1, buffer, sem)
    gates, select = gate_rows(meta_ref[0], ids, local * cap, top_k)
    select_ref[0] = select
    gate_ref[0] = jnp.broadcast_to(jnp.sum(gates, axis=1, keepdims=True), gate_ref.shape[1:])
    lay_rows(local, cap, dot(select, buffer[slot, 0]), xd_ref)


def dispatch_x(ids, blocks, meta_all, local, cap, top_k):
    tokens, dim = blocks[0].shape[-2:]
    groups = sum(block.shape[0] for block in blocks)
    rows = local * cap
    return pl.pallas_call(
        functools.partial(dispatch_x_kernel, local, cap, top_k),
        grid_spec=pltpu.PrefetchScalarGridSpec(
            num_scalar_prefetch=1, grid=(groups,),
            in_specs=[pl.BlockSpec(memory_space=pl.ANY)] * len(blocks)
            + [pl.BlockSpec((1, 2 * top_k, tokens), lambda s, ids: (ep_of(s, ids), 0, 0))],
            out_specs=[pl.BlockSpec((local, cap, dim), lambda s, ids: (0, s, 0)),
                       pl.BlockSpec((1, rows, tokens), lambda s, ids: (s, 0, 0)),
                       pl.BlockSpec((1, rows, 128), lambda s, ids: (s, 0, 0))],
            scratch_shapes=[pltpu.VMEM((2, 1, tokens, dim), BF16), pltpu.SemaphoreType.DMA((2, 1))]),
        out_shape=[jax.ShapeDtypeStruct((local, groups * cap, dim), BF16),
                   jax.ShapeDtypeStruct((groups, rows, tokens), BF16), jax.ShapeDtypeStruct((groups, rows, 128), F32)],
        compiler_params=params(1), name="dispatch_x",
        cost_estimate=pl.CostEstimate(flops=2 * groups * rows * tokens * dim,
                                      bytes_accessed=groups * (tokens + rows) * dim * 2, transcendentals=0),
    )(ids, *blocks, meta_all)


def dispatch_dy_kernel(local, cap, ids, dy_ref, select_ref, gate_ref, qd_ref):
    lay_rows(local, cap, dot(select_ref[0], dy_ref[0]) * gate_ref[0][:, :1], qd_ref)


def dispatch_dy(ids, dy_all, select, gate, local, cap):
    groups, tokens, dim = dy_all.shape
    rows = local * cap
    by_place = lambda s, ids: (s, 0, 0)
    return pl.pallas_call(
        functools.partial(dispatch_dy_kernel, local, cap),
        grid_spec=pltpu.PrefetchScalarGridSpec(
            num_scalar_prefetch=1, grid=(groups,),
            in_specs=[pl.BlockSpec((1, tokens, dim), lambda s, ids: (ep_of(s, ids), 0, 0)),
                      pl.BlockSpec((1, rows, tokens), by_place), pl.BlockSpec((1, rows, 128), by_place)],
            out_specs=pl.BlockSpec((local, cap, dim), lambda s, ids: (0, s, 0))),
        out_shape=jax.ShapeDtypeStruct((local, groups * cap, dim), BF16), compiler_params=params(1), name="dispatch_dy",
        cost_estimate=pl.CostEstimate(flops=2 * groups * rows * tokens * dim,
                                      bytes_accessed=groups * (tokens + rows) * dim * 2, transcendentals=0),
    )(ids, dy_all, select, gate)


def dispatch_far_kernel(local, cap, top_k, ids, *refs):
    *blocks, dy_ref, meta_ref, xd_ref, qd_ref, buffer, sem = refs
    slot = stream(blocks, 1, buffer, sem)
    gates, select = gate_rows(meta_ref[0], ids, local * cap, top_k)
    lay_rows(local, cap, dot(select, buffer[slot, 0]), xd_ref)
    lay_rows(local, cap, dot(select, dy_ref[0]) * jnp.sum(gates, axis=1, keepdims=True), qd_ref)


def dispatch_far(ids, blocks, dy_all, meta_all, local, cap, top_k):
    groups, tokens, dim = dy_all.shape
    by_ep = lambda s, ids: (ep_of(s, ids), 0, 0)
    out = jax.ShapeDtypeStruct((local, groups * cap, dim), BF16)
    out_spec = pl.BlockSpec((local, cap, dim), lambda s, ids: (0, s, 0))
    return pl.pallas_call(
        functools.partial(dispatch_far_kernel, local, cap, top_k),
        grid_spec=pltpu.PrefetchScalarGridSpec(
            num_scalar_prefetch=1, grid=(groups,),
            in_specs=[pl.BlockSpec(memory_space=pl.ANY)] * len(blocks)
            + [pl.BlockSpec((1, tokens, dim), by_ep), pl.BlockSpec((1, 2 * top_k, tokens), by_ep)],
            out_specs=[out_spec, out_spec],
            scratch_shapes=[pltpu.VMEM((2, 1, tokens, dim), BF16), pltpu.SemaphoreType.DMA((2, 1))]),
        out_shape=[out, out], compiler_params=params(1), name="dispatch_far",
        cost_estimate=pl.CostEstimate(flops=4 * groups * local * cap * tokens * dim,
                                      bytes_accessed=groups * (tokens + local * cap) * dim * 4, transcendentals=0),
    )(ids, *blocks, dy_all, meta_all)


def forward_kernel(cap, x_ref, w1_ref, w3_ref, w2_ref, o_ref, h_ref, a1_ref, a3_ref):
    rows = x_ref.shape[-2]
    half = rows // 2
    per = half // cap
    for part in range(2):
        span = slice(part * half, (part + 1) * half)
        x = x_ref[0, span]
        one, three = dot(x, w1_ref[0]), dot(x, w3_ref[0])
        hidden = (one * jax.nn.sigmoid(one) * three).astype(BF16)
        h_ref[0, span] = hidden
        a1_ref[0, span] = one
        a3_ref[0, span] = three
        out = dot(hidden, w2_ref[0])
        for s in range(per):
            o_ref[part * per + s] = out[s * cap:(s + 1) * cap].astype(BF16)


def forward(xd, w1, w3, w2, cap):
    local, rows, dim = xd.shape
    ff = w1.shape[-1]
    groups = rows // cap
    by_expert = lambda l: (l, 0, 0)
    hid_spec = pl.BlockSpec((1, rows, ff), by_expert)
    wide, tall = pl.BlockSpec((1, dim, ff), by_expert), pl.BlockSpec((1, ff, dim), by_expert)
    proj = jax.ShapeDtypeStruct((local, rows, ff), F32)
    return pl.pallas_call(
        functools.partial(forward_kernel, cap), grid=(local,),
        in_specs=[pl.BlockSpec((1, rows, dim), by_expert), wide, wide, tall],
        out_specs=[pl.BlockSpec((groups, cap, dim), lambda l: (0, l, 0)), hid_spec, hid_spec, hid_spec],
        out_shape=[jax.ShapeDtypeStruct((groups, local * cap, dim), BF16), jax.ShapeDtypeStruct((local, rows, ff), BF16),
                   proj, proj],
        compiler_params=params(1), name="forward",
        cost_estimate=pl.CostEstimate(flops=6 * local * rows * dim * ff,
                                      bytes_accessed=local * (4 * rows * dim + 10 * rows * ff + 6 * dim * ff),
                                      transcendentals=local * rows * ff),
    )(xd, w1, w3, w2)


def backward_kernel(cap, q_ref, a1_ref, a3_ref, w1_ref, w3_ref, w2_ref, dr_ref, da1_ref, da3_ref):
    rows = q_ref.shape[-2]
    half = rows // 2
    per = half // cap
    for part in range(2):
        span = slice(part * half, (part + 1) * half)
        _, da_one, da_three = swiglu_parts(a1_ref[0, span], a3_ref[0, span], dot_nt(q_ref[0, span], w2_ref[0]))
        da1_ref[0, span] = da_one
        da3_ref[0, span] = da_three
        grad = dot_nt(da_one, w1_ref[0]) + dot_nt(da_three, w3_ref[0])
        for s in range(per):
            dr_ref[part * per + s] = grad[s * cap:(s + 1) * cap].astype(BF16)


def backward(qd, a1, a3, w1, w3, w2, cap):
    local, rows, dim = qd.shape
    ff = w1.shape[-1]
    groups = rows // cap
    by_expert = lambda l: (l, 0, 0)
    hid_spec = pl.BlockSpec((1, rows, ff), by_expert)
    wide, tall = pl.BlockSpec((1, dim, ff), by_expert), pl.BlockSpec((1, ff, dim), by_expert)
    hid = jax.ShapeDtypeStruct((local, rows, ff), BF16)
    return pl.pallas_call(
        functools.partial(backward_kernel, cap), grid=(local,),
        in_specs=[pl.BlockSpec((1, rows, dim), by_expert), hid_spec, hid_spec, wide, wide, tall],
        out_specs=[pl.BlockSpec((groups, cap, dim), lambda l: (0, l, 0)), hid_spec, hid_spec],
        out_shape=[jax.ShapeDtypeStruct((groups, local * cap, dim), BF16), hid, hid],
        compiler_params=params(1), name="backward",
        cost_estimate=pl.CostEstimate(flops=6 * local * rows * dim * ff,
                                      bytes_accessed=local * (4 * rows * dim + 12 * rows * ff + 6 * dim * ff),
                                      transcendentals=local * rows * ff),
    )(qd, a1, a3, w1, w3, w2)


def grads_kernel(ids, x_ref, q_ref, xp_ref, qp_ref, h_ref, da1_ref, da3_ref, w1_ref, w3_ref, w2_ref,
                 g1_ref, g3_ref, g2_ref, rows_x, rows_q, hid, da_one, da_three, tall):
    rows = x_ref.shape[-2]
    half = rows // 2
    part = ids[0]
    width = g1_ref.shape[1]
    columns = pl.ds(pl.multiple_of(part * width, 128), width)
    ff = w1_ref.shape[-1]
    reach = tall.shape[0]
    chunk = pl.ds(pl.multiple_of(part * (ff - reach), 128), reach)
    rows_x[:rows] = x_ref[0, :, columns]
    rows_x[rows:] = xp_ref[0, :, columns]
    rows_q[:rows] = q_ref[0]
    rows_q[rows:] = qp_ref[0]
    hid[:rows] = h_ref[0]
    da_one[:rows] = da1_ref[0]
    da_three[:rows] = da3_ref[0]
    for piece in range(2):
        span = slice(piece * half, (piece + 1) * half)
        dest = slice(rows + piece * half, rows + (piece + 1) * half)
        x = xp_ref[0, span]
        hidden, one, three = swiglu_parts(dot(x, w1_ref[0]), dot(x, w3_ref[0]), dot_nt(qp_ref[0, span], w2_ref[0]))
        hid[dest] = hidden
        da_one[dest] = one
        da_three[dest] = three
    g1_ref[0] = dot_tn(rows_x[...], da_one[...]).astype(BF16)
    g3_ref[0] = dot_tn(rows_x[...], da_three[...]).astype(BF16)
    height = g2_ref.shape[1]
    tall[...] = dot_tn(hid[:, chunk], rows_q[...])
    skip = pl.multiple_of(part * (height - (ff - reach)), 8)
    g2_ref[0] = tall[pl.ds(skip, height)].astype(BF16)


def expert_grads(ids, xd, qd, xp, qp, h, da1, da3, w1, w3, w2, parts):
    local, rows, dim = xd.shape
    ff = w1.shape[-1]
    by_expert = lambda l, ids: (l, 0, 0)
    row_spec, hid_spec = pl.BlockSpec((1, rows, dim), by_expert), pl.BlockSpec((1, rows, ff), by_expert)
    wide, tall = pl.BlockSpec((1, dim, ff), by_expert), pl.BlockSpec((1, ff, dim), by_expert)
    g1 = jax.ShapeDtypeStruct((local, dim // parts, ff), BF16)
    g2 = jax.ShapeDtypeStruct((local, ff // parts, dim), BF16)
    g1_spec, g2_spec = pl.BlockSpec((1, dim // parts, ff), by_expert), pl.BlockSpec((1, ff // parts, dim), by_expert)
    reach = -(-(ff // parts) // 128) * 128
    return pl.pallas_call(
        grads_kernel,
        grid_spec=pltpu.PrefetchScalarGridSpec(
            num_scalar_prefetch=1, grid=(local,),
            in_specs=[row_spec, row_spec, row_spec, row_spec, hid_spec, hid_spec, hid_spec, wide, wide, tall],
            out_specs=[g1_spec, g1_spec, g2_spec],
            scratch_shapes=[pltpu.VMEM((2 * rows, dim // parts), BF16), pltpu.VMEM((2 * rows, dim), BF16)]
            + [pltpu.VMEM((2 * rows, ff), BF16)] * 3 + [pltpu.VMEM((reach, dim), F32)]),
        out_shape=[g1, g1, g2], compiler_params=params(1), name="grads",
        cost_estimate=pl.CostEstimate(flops=12 * local * rows * dim * ff,
                                      bytes_accessed=local * (8 * rows * dim + 6 * rows * ff + 9 * dim * ff),
                                      transcendentals=local * rows * ff),
    )(ids, xd, qd, xp, qp, h, da1, da3, w1, w3, w2)


def shared_kernel(ids, *refs):
    *blocks, dy_one_ref, dy_two_ref, wa_ref, wa_far_ref, w2_ref, w2_far_ref, h_ref, da_ref, g_ref, g_far_ref, buffer, sem = refs
    slot = stream(blocks, 2, buffer, sem)

    @pl.when(pl.program_id(0) == 0)
    def _():
        g_ref[...] = jnp.zeros_like(g_ref)
        g_far_ref[...] = jnp.zeros_like(g_far_ref)

    _, pair, tokens, dim = buffer.shape
    x = buffer[slot].reshape(pair * tokens, dim)
    dy = jnp.concatenate([dy_one_ref[0], dy_two_ref[0]], axis=0)
    for half, (grad_ref, up_ref, down_ref) in enumerate(((g_ref, wa_ref, w2_ref), (g_far_ref, wa_far_ref, w2_far_ref))):
        proj = dot(x, up_ref[...])
        hidden, da_one, da_three = swiglu_parts(proj[:, :SLICE], proj[:, SLICE:], dot_nt(dy, down_ref[...]))
        da = jnp.concatenate([da_one, da_three], axis=1)
        h_ref[:, :, half * SLICE:(half + 1) * SLICE] = hidden.reshape(pair, tokens, SLICE)
        da_ref[:, :, 2 * half * SLICE:2 * (half + 1) * SLICE] = da.reshape(pair, tokens, 2 * SLICE)
        grad_ref[:2 * SLICE] += dot_tn(da, x)
        grad_ref[2 * SLICE:] += dot_tn(hidden, dy)


def shared_expert(ids, blocks, dy_all, weights):
    groups, tokens, dim = dy_all.shape
    by_pair, fixed = lambda s, ids: (s, 0, 0), lambda s, ids: (0, 0)
    grad = jax.ShapeDtypeStruct((3 * SLICE, dim), F32)
    return pl.pallas_call(
        shared_kernel,
        grid_spec=pltpu.PrefetchScalarGridSpec(
            num_scalar_prefetch=1, grid=(groups // 2,),
            in_specs=[pl.BlockSpec(memory_space=pl.ANY)] * len(blocks)
            + [pl.BlockSpec((1, tokens, dim), lambda s, ids: (ep_of(2 * s, ids), 0, 0)),
               pl.BlockSpec((1, tokens, dim), lambda s, ids: (ep_of(2 * s + 1, ids), 0, 0)),
               ] + [pl.BlockSpec(weight.shape, fixed) for weight in weights],
            out_specs=[pl.BlockSpec((2, tokens, 2 * SLICE), by_pair), pl.BlockSpec((2, tokens, 4 * SLICE), by_pair),
                       pl.BlockSpec(grad.shape, fixed), pl.BlockSpec(grad.shape, fixed)],
            scratch_shapes=[pltpu.VMEM((2, 2, tokens, dim), BF16), pltpu.SemaphoreType.DMA((2, 2))]),
        out_shape=[jax.ShapeDtypeStruct((groups, tokens, 2 * SLICE), BF16),
                   jax.ShapeDtypeStruct((groups, tokens, 4 * SLICE), BF16), grad, grad],
        compiler_params=params(1), name="shared",
        cost_estimate=pl.CostEstimate(flops=18 * groups * tokens * dim * SLICE,
                                      bytes_accessed=4 * groups * tokens * dim, transcendentals=0),
    )(ids, *blocks, dy_all, dy_all, *weights)


def gate_matrix(meta, ids, rows, top_k):
    tokens = meta.shape[0]
    base = (ids[1] * rows).astype(F32)
    row_ids = lax.broadcasted_iota(jnp.int32, (tokens, rows), 1).astype(F32) + base
    gates = jnp.zeros((tokens, rows), F32)
    for j in range(top_k):
        gates = jnp.where(meta[:, j:j + 1] == row_ids, meta[:, top_k + j:top_k + j + 1], gates)
    return gates


def combine_out_kernel(top_k, ids, meta_ref, o_ref, h_ref, w2_ref, w2_far_ref, y_ref):
    tokens = h_ref.shape[1]
    gates = gate_matrix(meta_ref[0].T, ids, o_ref.shape[1], top_k)
    high = gates.astype(BF16)
    rest = gates - high.astype(F32)
    mid = rest.astype(BF16)
    low = (rest - mid.astype(F32)).astype(BF16)
    sums = dot(jnp.concatenate([high, mid, low], axis=0), o_ref[0])
    width = w2_ref.shape[0]
    y_ref[0] = (sums[:tokens] + sums[tokens:2 * tokens] + sums[2 * tokens:]
                + dot(h_ref[0, :, :width], w2_ref[...]) + dot(h_ref[0, :, width:], w2_far_ref[...]))


def combine_back_kernel(top_k, ids, meta_ref, dr_ref, da_ref, wa_ref, wa_far_ref, dx_ref):
    gates = gate_matrix(meta_ref[0].T, ids, dr_ref.shape[1], top_k)
    select = jnp.where(gates != 0.0, 1.0, 0.0).astype(BF16)
    width = wa_ref.shape[1]
    dx_ref[0] = (dot(select, dr_ref[0]) + dot_nt(da_ref[0, :, :width], wa_ref[...])
                 + dot_nt(da_ref[0, :, width:], wa_far_ref[...]))


def combine(kernel, ids, meta_all, returned, hidden, weights, top_k, passes):
    groups, rows, dim = returned.shape
    tokens, width = hidden.shape[1:]
    by_place = lambda s, ids: (s, 0, 0)
    by_ep = lambda s, ids: (ep_of(s, ids), 0, 0)
    return pl.pallas_call(
        functools.partial(kernel, top_k),
        grid_spec=pltpu.PrefetchScalarGridSpec(
            num_scalar_prefetch=1, grid=(groups,),
            in_specs=[pl.BlockSpec((1, 2 * top_k, tokens), by_ep), pl.BlockSpec((1, rows, dim), by_place),
                      pl.BlockSpec((1, tokens, width), by_place)]
            + [pl.BlockSpec(weight.shape, lambda s, ids: (0, 0)) for weight in weights],
            out_specs=pl.BlockSpec((1, tokens, dim), by_ep)),
        out_shape=jax.ShapeDtypeStruct((groups, tokens, dim), F32), compiler_params=params(1),
        cost_estimate=pl.CostEstimate(flops=2 * passes * groups * tokens * rows * dim,
                                      bytes_accessed=groups * (2 * rows + 4 * tokens) * dim, transcendentals=0),
    )(ids, meta_all, returned, hidden, *weights)


def finish_kernel(ids, near_ref, corner_ref, other_near_ref, other_corner_ref, g1_ref, g3_ref, g2_ref):
    def lay(ref):
        g1_ref[...] = ref[0, :SLICE].T
        g3_ref[...] = ref[0, SLICE:2 * SLICE].T
        g2_ref[...] = ref[0, 2 * SLICE:]

    device = pl.program_id(0)
    same = device % 2 == ids[1] % 2
    near = jnp.bitwise_xor(device // 2, ids[1] // 2) < 3
    pl.when(same & near)(lambda: lay(near_ref))
    pl.when(same & jnp.logical_not(near))(lambda: lay(corner_ref))
    pl.when(jnp.logical_not(same) & near)(lambda: lay(other_near_ref))
    pl.when(jnp.logical_not(same) & jnp.logical_not(near))(lambda: lay(other_corner_ref))


def finish(ids, slices, ff):
    _, height, dim = slices[0].shape
    near = pl.BlockSpec((1, height, dim), lambda e, ids: (jnp.minimum(jnp.bitwise_xor(e // 2, ids[1] // 2), 2), 0, 0))
    corner = pl.BlockSpec((1, height, dim), lambda e, ids: (0, 0, 0))
    wide, tall = jax.ShapeDtypeStruct((dim, ff), BF16), jax.ShapeDtypeStruct((ff, dim), BF16)
    return pl.pallas_call(
        finish_kernel,
        grid_spec=pltpu.PrefetchScalarGridSpec(
            num_scalar_prefetch=1, grid=(ff // SLICE,), in_specs=[near, corner, near, corner],
            out_specs=[pl.BlockSpec((dim, SLICE), lambda e, ids: (0, e)), pl.BlockSpec((dim, SLICE), lambda e, ids: (0, e)),
                       pl.BlockSpec((SLICE, dim), lambda e, ids: (e, 0))]),
        out_shape=[wide, wide, tall], compiler_params=params(1), name="finish",
        cost_estimate=pl.CostEstimate(flops=1_000_000_000, bytes_accessed=16 * height * dim * 2, transcendentals=0),
    )(ids, *slices)


def solution(mesh):
    ep_size, tp_size = mesh.shape["ep"], mesh.shape["tp"]
    row_spec = P(("ep", "tp"), None)
    expert_spec = P("ep", None, None)
    expert_grad_spec = P("ep", "tp", None)
    swap = [(0, 1), (1, 0)]
    cores, along_x, along_y = ([(i, i ^ bit) for i in range(ep_size)] for bit in (1, 2, 4))

    def move(value, axis, route):
        return lax.ppermute(value, axis, route)

    def device_fn(tokens, grad_y, expert_ids, gate_vals, slot_ids,
                  shared_w1, shared_w3, shared_w2, expert_w1, expert_w3, expert_w2):
        rows_dev, dim = tokens.shape
        top_k = expert_ids.shape[1]
        local = expert_w1.shape[0]
        experts = local * ep_size
        cap = (2 * rows_dev * top_k + experts - 1) // experts
        tp_id, ep_id = lax.axis_index("tp"), lax.axis_index("ep")
        ids = jnp.stack([tp_id, ep_id]).astype(jnp.int32)

        pos = jnp.where(slot_ids >= 0, expert_ids * cap + slot_ids, -1).astype(F32)
        meta = jnp.concatenate([pos.T, gate_vals.T], axis=0)
        near_x, near_y, *others, far_own, far_other, meta_all, late_dy = gather_layer(tokens, grad_y, meta, ep_size)
        blocks = (tokens[None], near_x, near_y, *others)
        dy_all = lax.all_gather(late_dy, "ep")
        far_dy_all = lax.all_gather(move(late_dy, "tp", swap), "ep")
        far_meta = move(meta_all, "tp", swap)
        far_x, far_y = move(near_x, "tp", swap), move(near_y, "tp", swap)
        far_blocks = (far_own, far_x, far_y, far_other, move(far_x, "ep", cores), move(far_y, "ep", cores))

        ff = shared_w1.shape[1]
        padded = ep_size * SLICE
        wide_pad = ((0, 0), (0, padded - ff))
        start = ep_id * SLICE
        w1s = lax.dynamic_slice(jnp.pad(shared_w1, wide_pad), (0, start), (dim, SLICE))
        w3s = lax.dynamic_slice(jnp.pad(shared_w3, wide_pad), (0, start), (dim, SLICE))
        w2s = lax.dynamic_slice(jnp.pad(shared_w2, ((0, padded - ff), (0, 0))), (start, 0), (SLICE, dim))
        wa_own = jnp.concatenate([w1s, w3s], axis=1)
        wide = (wa_own, move(wa_own, "tp", swap))
        tall = (w2s, move(w2s, "tp", swap))

        sizes = (local, cap, top_k)
        xd, rows_select, rows_gate = dispatch_x(ids, blocks, meta_all, *sizes)
        o, h, a1, a3 = forward(xd, expert_w1, expert_w3, expert_w2, cap)
        qd = dispatch_dy(ids, dy_all, rows_select, rows_gate, local, cap)
        sh, sda, shared_grad, shared_far = shared_expert(ids, blocks, dy_all, wide + tall)
        y_part = combine(combine_out_kernel, ids, meta_all, o, sh, tall, top_k, 3)
        y_sum = lax.psum_scatter(y_part.reshape(-1, dim), "ep", scatter_dimension=0, tiled=True)
        dr, da1, da3 = backward(qd, a1, a3, expert_w1, expert_w3, expert_w2, cap)
        dx_part = combine(combine_back_kernel, ids, meta_all, dr, sda, wide, top_k, 1)
        dx_sum = lax.psum_scatter(dx_part.reshape(-1, dim), "ep", scatter_dimension=0, tiled=True)

        xp, qp = dispatch_far(ids, far_blocks, far_dy_all, far_meta, *sizes)
        g1, g3, g2 = expert_grads(ids, xd, qd, xp, qp, h, da1, da3, expert_w1, expert_w3, expert_w2, tp_size)

        shared_grad = shared_grad + move(shared_far, "tp", swap)
        mine = shared_grad.astype(BF16)
        from_x, from_y = move(mine, "ep", along_x), move(mine, "ep", along_y)
        chips = jnp.stack([mine, from_x, from_y])
        corner = move(from_x, "ep", along_y)
        slices = (chips, corner[None], move(chips, "ep", cores), move(corner, "ep", cores)[None])
        sg1, sg3, sg2 = finish(ids, slices, ff)
        out_y = (tokens.astype(F32) + y_sum).astype(BF16)
        grad_tokens = (grad_y.astype(F32) + dx_sum).astype(BF16)
        return out_y, grad_tokens, sg1, sg3, sg2, g1, g3, g2

    return jax.shard_map(
        device_fn, mesh=mesh,
        in_specs=(row_spec, row_spec, row_spec, row_spec, row_spec,
                  P(None, "tp"), P(None, "tp"), P("tp", None), expert_spec, expert_spec, expert_spec),
        out_specs=(row_spec, row_spec, P(None, "tp"), P(None, "tp"), P("tp", None),
                   expert_grad_spec, expert_grad_spec, expert_grad_spec),
        check_vma=False)
```

```python
import functools

import jax
import jax.numpy as jnp
from jax import lax
from jax.experimental import pallas as pl
from jax.experimental.pallas import tpu as pltpu
from jax.sharding import PartitionSpec as P


F32 = jnp.float32
BF16 = jnp.bfloat16
SLICE = 128
VMEM_LIMIT = 64_000_000
MESH = pl.DeviceIdType.MESH
NT = (((1,), (1,)), ((), ()))
TN = (((0,), (0,)), ((), ()))


def dot(a, b):
    return jnp.dot(a, b, preferred_element_type=F32)


def dot_nt(a, b):
    return lax.dot_general(a, b, NT, preferred_element_type=F32)


def dot_tn(a, b):
    return lax.dot_general(a, b, TN, preferred_element_type=F32)


def swiglu_parts(one, three, grad_hidden):
    sig = jax.nn.sigmoid(one)
    silu = one * sig
    dh = grad_hidden.astype(BF16).astype(F32)
    hidden = (silu * three).astype(BF16)
    da_one = (dh * three * (sig + silu * (1.0 - sig))).astype(BF16)
    da_three = (dh * silu).astype(BF16)
    return hidden, da_one, da_three


def params(axes):
    return pltpu.CompilerParams(dimension_semantics=("arbitrary",) * axes, vmem_limit_bytes=VMEM_LIMIT)


def gather_kernel(ep_size, x_ref, dy_ref, meta_ref, near_x_ref, near_y_ref, other_own_ref, other_x_ref, other_y_ref,
                  far_own_ref, far_other_ref, meta_all_ref, dy_out_ref, mine, mine_dy, mine_meta,
                  load_sem, store_sem, send_sem, recv_sem):
    me = lax.axis_index("ep")
    core_peer = me + 1 - 2 * (me % 2)
    x_peer = me + 2 - 4 * ((me // 2) % 2)
    y_peer = me + 4 - 8 * (me // 4)
    z_peer = 1 - lax.axis_index("tp")

    barrier = pltpu.get_barrier_semaphore()
    for k in range(1, ep_size):
        pl.semaphore_signal(barrier, inc=1, device_id={"ep": (me + k) % ep_size}, device_id_type=MESH)
    pl.semaphore_signal(barrier, inc=1, device_id={"tp": z_peer}, device_id_type=MESH)

    loads = [pltpu.make_async_copy(x_ref, mine, load_sem.at[0]),
             pltpu.make_async_copy(meta_ref, mine_meta, load_sem.at[1]),
             pltpu.make_async_copy(dy_ref, mine_dy, load_sem.at[2])]
    for copy in loads:
        copy.start()
    for copy in loads:
        copy.wait()
    stores = [pltpu.make_async_copy(mine_dy, dy_out_ref, store_sem.at[0]),
              pltpu.make_async_copy(mine_meta, meta_all_ref.at[me], store_sem.at[1])]
    pl.semaphore_wait(barrier, ep_size)

    half = x_ref.shape[0] // 2
    low, high = pl.ds(0, half), pl.ds(half, half)
    started = []

    def send(device, src, dst):
        n = len(started)
        copy = pltpu.make_async_remote_copy(src_ref=src, dst_ref=dst, send_sem=send_sem.at[n], recv_sem=recv_sem.at[n],
                                            device_id=device, device_id_type=MESH)
        copy.start()
        started.append(copy)
        return copy

    to_x, to_y, to_core = {"ep": x_peer}, {"ep": y_peer}, {"ep": core_peer}
    from_x_low = send(to_x, mine.at[low], near_x_ref.at[0, low])
    from_y_high = send(to_y, mine.at[high], near_y_ref.at[0, high])
    from_z = send({"tp": z_peer}, mine, far_own_ref.at[0])
    from_x_high = send(to_x, mine.at[high], near_x_ref.at[0, high])
    from_y_low = send(to_y, mine.at[low], near_y_ref.at[0, low])
    waiting = [send({"ep": (me + k) % ep_size}, mine_meta, meta_all_ref.at[me]) for k in range(1, ep_size)]
    waiting.append(send(to_core, mine, other_own_ref.at[0]))
    for copy in stores:
        copy.start()
    from_x_low.wait_recv()
    corner_low = send(to_y, near_x_ref.at[0, low], near_y_ref.at[1, low])
    waiting.append(send(to_core, near_x_ref.at[0, low], other_x_ref.at[0, low]))
    from_y_high.wait_recv()
    corner_high = send(to_x, near_y_ref.at[0, high], near_y_ref.at[1, high])
    waiting.append(send(to_core, near_y_ref.at[0, high], other_y_ref.at[0, high]))
    from_x_high.wait_recv()
    waiting.append(send(to_core, near_x_ref.at[0, high], other_x_ref.at[0, high]))
    from_y_low.wait_recv()
    waiting.append(send(to_core, near_y_ref.at[0, low], other_y_ref.at[0, low]))
    from_z.wait_recv()
    waiting.append(send(to_core, far_own_ref.at[0], far_other_ref.at[0]))
    corner_low.wait_recv()
    waiting.append(send(to_core, near_y_ref.at[1, low], other_y_ref.at[1, low]))
    corner_high.wait_recv()
    waiting.append(send(to_core, near_y_ref.at[1, high], other_y_ref.at[1, high]))
    for copy in waiting:
        copy.wait_recv()
    for copy in started:
        copy.wait_send()
    for copy in stores:
        copy.wait()


def gather_layer(tokens, grad_y, meta, ep_size):
    rows, dim = tokens.shape
    one = jax.ShapeDtypeStruct((1, rows, dim), tokens.dtype)
    two = jax.ShapeDtypeStruct((2, rows, dim), tokens.dtype)
    anywhere = pl.BlockSpec(memory_space=pl.ANY)
    copies = 5 + (ep_size - 1) + 1 + 2 + 7
    return pl.pallas_call(
        functools.partial(gather_kernel, ep_size),
        in_specs=[anywhere] * 3, out_specs=[anywhere] * 9,
        out_shape=[one, two, one, one, two, one, one, jax.ShapeDtypeStruct((ep_size,) + meta.shape, meta.dtype),
                   jax.ShapeDtypeStruct(grad_y.shape, grad_y.dtype)],
        scratch_shapes=[pltpu.VMEM((rows, dim), tokens.dtype), pltpu.VMEM((rows, dim), grad_y.dtype),
                        pltpu.VMEM(meta.shape, meta.dtype), pltpu.SemaphoreType.DMA((3,)), pltpu.SemaphoreType.DMA((2,)),
                        pltpu.SemaphoreType.DMA((copies,)), pltpu.SemaphoreType.DMA((copies,))],
        compiler_params=pltpu.CompilerParams(collective_id=0, has_side_effects=True), name="gather",
        cost_estimate=pl.CostEstimate(flops=30_000_000_000, bytes_accessed=ep_size * rows * dim * 8, transcendentals=0),
    )(tokens, grad_y, meta)


def ep_of(source, ids):
    core = jnp.where(source < 4, ids[1] % 2, 1 - ids[1] % 2)
    return 2 * jnp.bitwise_xor(ids[1] // 2, source % 4) + core


def stream(refs, per_step, buffer, sem):
    blocks = [(ref, i) for ref in refs for i in range(ref.shape[0])]
    step = pl.program_id(0)
    steps = len(blocks) // per_step

    def copies(k):
        return [pltpu.make_async_copy(ref.at[i], buffer.at[k % 2, n], sem.at[k % 2, n])
                for n, (ref, i) in enumerate(blocks[k * per_step:(k + 1) * per_step])]

    @pl.when(step == 0)
    def _():
        for copy in copies(0):
            copy.start()

    for k in range(steps):
        @pl.when(step == k)
        def _():
            if k + 1 < steps:
                for copy in copies(k + 1):
                    copy.start()
            for copy in copies(k):
                copy.wait()

    return step % 2


def lay_rows(local, cap, got, out_ref):
    for l in range(local):
        out_ref[l] = got[l * cap:(l + 1) * cap].astype(BF16)


def gate_rows(meta, ids, rows, top_k):
    tokens = meta.shape[1]
    base = (ids[1] * rows).astype(F32)
    row_ids = lax.broadcasted_iota(jnp.int32, (rows, tokens), 0).astype(F32) + base
    gates = jnp.zeros((rows, tokens), F32)
    for j in range(top_k):
        gates = jnp.where(meta[j][None, :] == row_ids, meta[top_k + j][None, :], gates)
    return gates, jnp.where(gates != 0.0, 1.0, 0.0).astype(BF16)


def dispatch_x_kernel(local, cap, top_k, ids, *refs):
    *blocks, meta_ref, xd_ref, select_ref, gate_ref, buffer, sem = refs
    slot = stream(blocks, 1, buffer, sem)
    gates, select = gate_rows(meta_ref[0], ids, local * cap, top_k)
    select_ref[0] = select
    gate_ref[0] = jnp.broadcast_to(jnp.sum(gates, axis=1, keepdims=True), gate_ref.shape[1:])
    lay_rows(local, cap, dot(select, buffer[slot, 0]), xd_ref)


def dispatch_x(ids, blocks, meta_all, local, cap, top_k):
    tokens, dim = blocks[0].shape[-2:]
    groups = sum(block.shape[0] for block in blocks)
    rows = local * cap
    return pl.pallas_call(
        functools.partial(dispatch_x_kernel, local, cap, top_k),
        grid_spec=pltpu.PrefetchScalarGridSpec(
            num_scalar_prefetch=1, grid=(groups,),
            in_specs=[pl.BlockSpec(memory_space=pl.ANY)] * len(blocks)
            + [pl.BlockSpec((1, 2 * top_k, tokens), lambda s, ids: (ep_of(s, ids), 0, 0))],
            out_specs=[pl.BlockSpec((local, cap, dim), lambda s, ids: (0, s, 0)),
                       pl.BlockSpec((1, rows, tokens), lambda s, ids: (s, 0, 0)),
                       pl.BlockSpec((1, rows, 128), lambda s, ids: (s, 0, 0))],
            scratch_shapes=[pltpu.VMEM((2, 1, tokens, dim), BF16), pltpu.SemaphoreType.DMA((2, 1))]),
        out_shape=[jax.ShapeDtypeStruct((local, groups * cap, dim), BF16),
                   jax.ShapeDtypeStruct((groups, rows, tokens), BF16), jax.ShapeDtypeStruct((groups, rows, 128), F32)],
        compiler_params=params(1), name="dispatch_x",
        cost_estimate=pl.CostEstimate(flops=2 * groups * rows * tokens * dim,
                                      bytes_accessed=groups * (tokens + rows) * dim * 2, transcendentals=0),
    )(ids, *blocks, meta_all)


def dispatch_dy_kernel(local, cap, ids, dy_ref, select_ref, gate_ref, qd_ref):
    lay_rows(local, cap, dot(select_ref[0], dy_ref[0]) * gate_ref[0][:, :1], qd_ref)


def dispatch_dy(ids, dy_all, select, gate, local, cap):
    groups, tokens, dim = dy_all.shape
    rows = local * cap
    by_place = lambda s, ids: (s, 0, 0)
    return pl.pallas_call(
        functools.partial(dispatch_dy_kernel, local, cap),
        grid_spec=pltpu.PrefetchScalarGridSpec(
            num_scalar_prefetch=1, grid=(groups,),
            in_specs=[pl.BlockSpec((1, tokens, dim), lambda s, ids: (ep_of(s, ids), 0, 0)),
                      pl.BlockSpec((1, rows, tokens), by_place), pl.BlockSpec((1, rows, 128), by_place)],
            out_specs=pl.BlockSpec((local, cap, dim), lambda s, ids: (0, s, 0))),
        out_shape=jax.ShapeDtypeStruct((local, groups * cap, dim), BF16), compiler_params=params(1), name="dispatch_dy",
        cost_estimate=pl.CostEstimate(flops=2 * groups * rows * tokens * dim,
                                      bytes_accessed=groups * (tokens + rows) * dim * 2, transcendentals=0),
    )(ids, dy_all, select, gate)


def dispatch_far_kernel(local, cap, top_k, ids, *refs):
    *blocks, dy_ref, meta_ref, xd_ref, qd_ref, buffer, sem = refs
    slot = stream(blocks, 1, buffer, sem)
    gates, select = gate_rows(meta_ref[0], ids, local * cap, top_k)
    lay_rows(local, cap, dot(select, buffer[slot, 0]), xd_ref)
    lay_rows(local, cap, dot(select, dy_ref[0]) * jnp.sum(gates, axis=1, keepdims=True), qd_ref)


def dispatch_far(ids, blocks, dy_all, meta_all, local, cap, top_k):
    groups, tokens, dim = dy_all.shape
    by_ep = lambda s, ids: (ep_of(s, ids), 0, 0)
    out = jax.ShapeDtypeStruct((local, groups * cap, dim), BF16)
    out_spec = pl.BlockSpec((local, cap, dim), lambda s, ids: (0, s, 0))
    return pl.pallas_call(
        functools.partial(dispatch_far_kernel, local, cap, top_k),
        grid_spec=pltpu.PrefetchScalarGridSpec(
            num_scalar_prefetch=1, grid=(groups,),
            in_specs=[pl.BlockSpec(memory_space=pl.ANY)] * len(blocks)
            + [pl.BlockSpec((1, tokens, dim), by_ep), pl.BlockSpec((1, 2 * top_k, tokens), by_ep)],
            out_specs=[out_spec, out_spec],
            scratch_shapes=[pltpu.VMEM((2, 1, tokens, dim), BF16), pltpu.SemaphoreType.DMA((2, 1))]),
        out_shape=[out, out], compiler_params=params(1), name="dispatch_far",
        cost_estimate=pl.CostEstimate(flops=4 * groups * local * cap * tokens * dim,
                                      bytes_accessed=groups * (tokens + local * cap) * dim * 4, transcendentals=0),
    )(ids, *blocks, dy_all, meta_all)


def forward_kernel(cap, x_ref, w1_ref, w3_ref, w2_ref, o_ref, h_ref, a1_ref, a3_ref):
    rows = x_ref.shape[-2]
    half = rows // 2
    per = half // cap
    for part in range(2):
        span = slice(part * half, (part + 1) * half)
        x = x_ref[0, span]
        one, three = dot(x, w1_ref[0]), dot(x, w3_ref[0])
        hidden = (one * jax.nn.sigmoid(one) * three).astype(BF16)
        h_ref[0, span] = hidden
        a1_ref[0, span] = one
        a3_ref[0, span] = three
        out = dot(hidden, w2_ref[0])
        for s in range(per):
            o_ref[part * per + s] = out[s * cap:(s + 1) * cap].astype(BF16)


def forward(xd, w1, w3, w2, cap):
    local, rows, dim = xd.shape
    ff = w1.shape[-1]
    groups = rows // cap
    by_expert = lambda l: (l, 0, 0)
    hid_spec = pl.BlockSpec((1, rows, ff), by_expert)
    wide, tall = pl.BlockSpec((1, dim, ff), by_expert), pl.BlockSpec((1, ff, dim), by_expert)
    proj = jax.ShapeDtypeStruct((local, rows, ff), F32)
    return pl.pallas_call(
        functools.partial(forward_kernel, cap), grid=(local,),
        in_specs=[pl.BlockSpec((1, rows, dim), by_expert), wide, wide, tall],
        out_specs=[pl.BlockSpec((groups, cap, dim), lambda l: (0, l, 0)), hid_spec, hid_spec, hid_spec],
        out_shape=[jax.ShapeDtypeStruct((groups, local * cap, dim), BF16), jax.ShapeDtypeStruct((local, rows, ff), BF16),
                   proj, proj],
        compiler_params=params(1), name="forward",
        cost_estimate=pl.CostEstimate(flops=6 * local * rows * dim * ff,
                                      bytes_accessed=local * (4 * rows * dim + 10 * rows * ff + 6 * dim * ff),
                                      transcendentals=local * rows * ff),
    )(xd, w1, w3, w2)


def backward_kernel(cap, q_ref, a1_ref, a3_ref, w1_ref, w3_ref, w2_ref, dr_ref, da1_ref, da3_ref):
    rows = q_ref.shape[-2]
    half = rows // 2
    per = half // cap
    for part in range(2):
        span = slice(part * half, (part + 1) * half)
        _, da_one, da_three = swiglu_parts(a1_ref[0, span], a3_ref[0, span], dot_nt(q_ref[0, span], w2_ref[0]))
        da1_ref[0, span] = da_one
        da3_ref[0, span] = da_three
        grad = dot_nt(da_one, w1_ref[0]) + dot_nt(da_three, w3_ref[0])
        for s in range(per):
            dr_ref[part * per + s] = grad[s * cap:(s + 1) * cap].astype(BF16)


def backward(qd, a1, a3, w1, w3, w2, cap):
    local, rows, dim = qd.shape
    ff = w1.shape[-1]
    groups = rows // cap
    by_expert = lambda l: (l, 0, 0)
    hid_spec = pl.BlockSpec((1, rows, ff), by_expert)
    wide, tall = pl.BlockSpec((1, dim, ff), by_expert), pl.BlockSpec((1, ff, dim), by_expert)
    hid = jax.ShapeDtypeStruct((local, rows, ff), BF16)
    return pl.pallas_call(
        functools.partial(backward_kernel, cap), grid=(local,),
        in_specs=[pl.BlockSpec((1, rows, dim), by_expert), hid_spec, hid_spec, wide, wide, tall],
        out_specs=[pl.BlockSpec((groups, cap, dim), lambda l: (0, l, 0)), hid_spec, hid_spec],
        out_shape=[jax.ShapeDtypeStruct((groups, local * cap, dim), BF16), hid, hid],
        compiler_params=params(1), name="backward",
        cost_estimate=pl.CostEstimate(flops=6 * local * rows * dim * ff,
                                      bytes_accessed=local * (4 * rows * dim + 12 * rows * ff + 6 * dim * ff),
                                      transcendentals=local * rows * ff),
    )(qd, a1, a3, w1, w3, w2)


def grads_kernel(ids, x_ref, q_ref, xp_ref, qp_ref, h_ref, da1_ref, da3_ref, w1_ref, w3_ref, w2_ref,
                 g1_ref, g3_ref, g2_ref, rows_x, rows_q, hid, da_one, da_three, tall):
    rows = x_ref.shape[-2]
    half = rows // 2
    part = ids[0]
    width = g1_ref.shape[1]
    columns = pl.ds(pl.multiple_of(part * width, 128), width)
    ff = w1_ref.shape[-1]
    reach = tall.shape[0]
    chunk = pl.ds(pl.multiple_of(part * (ff - reach), 128), reach)
    rows_x[:rows] = x_ref[0, :, columns]
    rows_x[rows:] = xp_ref[0, :, columns]
    rows_q[:rows] = q_ref[0]
    rows_q[rows:] = qp_ref[0]
    hid[:rows] = h_ref[0]
    da_one[:rows] = da1_ref[0]
    da_three[:rows] = da3_ref[0]
    for piece in range(2):
        span = slice(piece * half, (piece + 1) * half)
        dest = slice(rows + piece * half, rows + (piece + 1) * half)
        x = xp_ref[0, span]
        hidden, one, three = swiglu_parts(dot(x, w1_ref[0]), dot(x, w3_ref[0]), dot_nt(qp_ref[0, span], w2_ref[0]))
        hid[dest] = hidden
        da_one[dest] = one
        da_three[dest] = three
    g1_ref[0] = dot_tn(rows_x[...], da_one[...]).astype(BF16)
    g3_ref[0] = dot_tn(rows_x[...], da_three[...]).astype(BF16)
    height = g2_ref.shape[1]
    tall[...] = dot_tn(hid[:, chunk], rows_q[...])
    skip = pl.multiple_of(part * (height - (ff - reach)), 8)
    g2_ref[0] = tall[pl.ds(skip, height)].astype(BF16)


def expert_grads(ids, xd, qd, xp, qp, h, da1, da3, w1, w3, w2, parts):
    local, rows, dim = xd.shape
    ff = w1.shape[-1]
    by_expert = lambda l, ids: (l, 0, 0)
    row_spec, hid_spec = pl.BlockSpec((1, rows, dim), by_expert), pl.BlockSpec((1, rows, ff), by_expert)
    wide, tall = pl.BlockSpec((1, dim, ff), by_expert), pl.BlockSpec((1, ff, dim), by_expert)
    g1 = jax.ShapeDtypeStruct((local, dim // parts, ff), BF16)
    g2 = jax.ShapeDtypeStruct((local, ff // parts, dim), BF16)
    g1_spec, g2_spec = pl.BlockSpec((1, dim // parts, ff), by_expert), pl.BlockSpec((1, ff // parts, dim), by_expert)
    reach = -(-(ff // parts) // 128) * 128
    return pl.pallas_call(
        grads_kernel,
        grid_spec=pltpu.PrefetchScalarGridSpec(
            num_scalar_prefetch=1, grid=(local,),
            in_specs=[row_spec, row_spec, row_spec, row_spec, hid_spec, hid_spec, hid_spec, wide, wide, tall],
            out_specs=[g1_spec, g1_spec, g2_spec],
            scratch_shapes=[pltpu.VMEM((2 * rows, dim // parts), BF16), pltpu.VMEM((2 * rows, dim), BF16)]
            + [pltpu.VMEM((2 * rows, ff), BF16)] * 3 + [pltpu.VMEM((reach, dim), F32)]),
        out_shape=[g1, g1, g2], compiler_params=params(1), name="grads",
        cost_estimate=pl.CostEstimate(flops=12 * local * rows * dim * ff,
                                      bytes_accessed=local * (8 * rows * dim + 6 * rows * ff + 9 * dim * ff),
                                      transcendentals=local * rows * ff),
    )(ids, xd, qd, xp, qp, h, da1, da3, w1, w3, w2)


def shared_kernel(ids, *refs):
    *blocks, dy_one_ref, dy_two_ref, wa_ref, wa_far_ref, w2_ref, w2_far_ref, h_ref, da_ref, g_ref, g_far_ref, buffer, sem = refs
    slot = stream(blocks, 2, buffer, sem)

    @pl.when(pl.program_id(0) == 0)
    def _():
        g_ref[...] = jnp.zeros_like(g_ref)
        g_far_ref[...] = jnp.zeros_like(g_far_ref)

    _, pair, tokens, dim = buffer.shape
    x = buffer[slot].reshape(pair * tokens, dim)
    dy = jnp.concatenate([dy_one_ref[0], dy_two_ref[0]], axis=0)
    for half, (grad_ref, up_ref, down_ref) in enumerate(((g_ref, wa_ref, w2_ref), (g_far_ref, wa_far_ref, w2_far_ref))):
        proj = dot(x, up_ref[...])
        hidden, da_one, da_three = swiglu_parts(proj[:, :SLICE], proj[:, SLICE:], dot_nt(dy, down_ref[...]))
        da = jnp.concatenate([da_one, da_three], axis=1)
        h_ref[:, :, half * SLICE:(half + 1) * SLICE] = hidden.reshape(pair, tokens, SLICE)
        da_ref[:, :, 2 * half * SLICE:2 * (half + 1) * SLICE] = da.reshape(pair, tokens, 2 * SLICE)
        grad_ref[:2 * SLICE] += dot_tn(da, x)
        grad_ref[2 * SLICE:] += dot_tn(hidden, dy)


def shared_expert(ids, blocks, dy_all, weights):
    groups, tokens, dim = dy_all.shape
    by_pair, fixed = lambda s, ids: (s, 0, 0), lambda s, ids: (0, 0)
    grad = jax.ShapeDtypeStruct((3 * SLICE, dim), F32)
    return pl.pallas_call(
        shared_kernel,
        grid_spec=pltpu.PrefetchScalarGridSpec(
            num_scalar_prefetch=1, grid=(groups // 2,),
            in_specs=[pl.BlockSpec(memory_space=pl.ANY)] * len(blocks)
            + [pl.BlockSpec((1, tokens, dim), lambda s, ids: (ep_of(2 * s, ids), 0, 0)),
               pl.BlockSpec((1, tokens, dim), lambda s, ids: (ep_of(2 * s + 1, ids), 0, 0)),
               ] + [pl.BlockSpec(weight.shape, fixed) for weight in weights],
            out_specs=[pl.BlockSpec((2, tokens, 2 * SLICE), by_pair), pl.BlockSpec((2, tokens, 4 * SLICE), by_pair),
                       pl.BlockSpec(grad.shape, fixed), pl.BlockSpec(grad.shape, fixed)],
            scratch_shapes=[pltpu.VMEM((2, 2, tokens, dim), BF16), pltpu.SemaphoreType.DMA((2, 2))]),
        out_shape=[jax.ShapeDtypeStruct((groups, tokens, 2 * SLICE), BF16),
                   jax.ShapeDtypeStruct((groups, tokens, 4 * SLICE), BF16), grad, grad],
        compiler_params=params(1), name="shared",
        cost_estimate=pl.CostEstimate(flops=18 * groups * tokens * dim * SLICE,
                                      bytes_accessed=4 * groups * tokens * dim, transcendentals=0),
    )(ids, *blocks, dy_all, dy_all, *weights)


def gate_matrix(meta, ids, rows, top_k):
    tokens = meta.shape[0]
    base = (ids[1] * rows).astype(F32)
    row_ids = lax.broadcasted_iota(jnp.int32, (tokens, rows), 1).astype(F32) + base
    gates = jnp.zeros((tokens, rows), F32)
    for j in range(top_k):
        gates = jnp.where(meta[:, j:j + 1] == row_ids, meta[:, top_k + j:top_k + j + 1], gates)
    return gates


def combine_out_kernel(top_k, ids, meta_ref, o_ref, h_ref, w2_ref, w2_far_ref, y_ref, select_ref):
    tokens = h_ref.shape[1]
    meta = meta_ref[0].T
    width = w2_ref.shape[0]
    part = tokens // 2
    for first in range(0, tokens, part):
        span = slice(first, first + part)
        gates = gate_matrix(meta[span], ids, o_ref.shape[1], top_k)
        select_ref[0, span] = jnp.where(gates != 0.0, 1.0, 0.0).astype(BF16)
        high = gates.astype(BF16)
        rest = gates - high.astype(F32)
        mid = rest.astype(BF16)
        low = (rest - mid.astype(F32)).astype(BF16)
        sums = dot(jnp.concatenate([high, mid, low], axis=0), o_ref[0])
        y_ref[0, span] = (sums[:part] + sums[part:2 * part] + sums[2 * part:]
                          + dot(h_ref[0, span, :width], w2_ref[...]) + dot(h_ref[0, span, width:], w2_far_ref[...]))


def combine_out(ids, meta_all, o, h, weights, top_k):
    groups, rows, dim = o.shape
    tokens, width = h.shape[1:]
    by_place = lambda s, ids: (s, 0, 0)
    by_ep = lambda s, ids: (ep_of(s, ids), 0, 0)
    return pl.pallas_call(
        functools.partial(combine_out_kernel, top_k),
        grid_spec=pltpu.PrefetchScalarGridSpec(
            num_scalar_prefetch=1, grid=(groups,),
            in_specs=[pl.BlockSpec((1, 2 * top_k, tokens), by_ep), pl.BlockSpec((1, rows, dim), by_place),
                      pl.BlockSpec((1, tokens, width), by_place)]
            + [pl.BlockSpec(weight.shape, lambda s, ids: (0, 0)) for weight in weights],
            out_specs=[pl.BlockSpec((1, tokens, dim), by_ep), pl.BlockSpec((1, tokens, rows), by_place)]),
        out_shape=[jax.ShapeDtypeStruct((groups, tokens, dim), F32), jax.ShapeDtypeStruct((groups, tokens, rows), BF16)],
        compiler_params=params(1), name="combine_out",
        cost_estimate=pl.CostEstimate(flops=6 * groups * tokens * rows * dim,
                                      bytes_accessed=groups * (2 * rows + 4 * tokens) * dim, transcendentals=0),
    )(ids, meta_all, o, h, *weights)


def combine_back_kernel(ids, select_ref, dr_ref, da_ref, wa_ref, wa_far_ref, dx_ref):
    width = wa_ref.shape[1]
    dx_ref[0] = (dot(select_ref[0], dr_ref[0]) + dot_nt(da_ref[0, :, :width], wa_ref[...])
                 + dot_nt(da_ref[0, :, width:], wa_far_ref[...]))


def combine_back(ids, select, dr, da, weights):
    groups, rows, dim = dr.shape
    tokens, width = da.shape[1:]
    by_place = lambda s, ids: (s, 0, 0)
    return pl.pallas_call(
        combine_back_kernel,
        grid_spec=pltpu.PrefetchScalarGridSpec(
            num_scalar_prefetch=1, grid=(groups,),
            in_specs=[pl.BlockSpec((1, tokens, rows), by_place), pl.BlockSpec((1, rows, dim), by_place),
                      pl.BlockSpec((1, tokens, width), by_place)]
            + [pl.BlockSpec(weight.shape, lambda s, ids: (0, 0)) for weight in weights],
            out_specs=pl.BlockSpec((1, tokens, dim), lambda s, ids: (ep_of(s, ids), 0, 0))),
        out_shape=jax.ShapeDtypeStruct((groups, tokens, dim), F32), compiler_params=params(1), name="combine_back",
        cost_estimate=pl.CostEstimate(flops=2 * groups * tokens * (rows + width) * dim,
                                      bytes_accessed=groups * (2 * rows + 4 * tokens) * dim, transcendentals=0),
    )(ids, select, dr, da, *weights)


def finish_kernel(ids, near_ref, corner_ref, other_near_ref, other_corner_ref, g1_ref, g3_ref, g2_ref):
    device = pl.program_id(0)
    place = pl.ds(pl.multiple_of(device * SLICE, SLICE), SLICE)

    def lay(ref):
        g1_ref[:, place] = ref[0, :SLICE].T
        g3_ref[:, place] = ref[0, SLICE:2 * SLICE].T
        g2_ref[place] = ref[0, 2 * SLICE:]

    same = device % 2 == ids[1] % 2
    near = jnp.bitwise_xor(device // 2, ids[1] // 2) < 3
    pl.when(same & near)(lambda: lay(near_ref))
    pl.when(same & jnp.logical_not(near))(lambda: lay(corner_ref))
    pl.when(jnp.logical_not(same) & near)(lambda: lay(other_near_ref))
    pl.when(jnp.logical_not(same) & jnp.logical_not(near))(lambda: lay(other_corner_ref))


def finish(ids, slices, ff):
    _, height, dim = slices[0].shape
    near = pl.BlockSpec((1, height, dim), lambda e, ids: (jnp.minimum(jnp.bitwise_xor(e // 2, ids[1] // 2), 2), 0, 0))
    corner = pl.BlockSpec((1, height, dim), lambda e, ids: (0, 0, 0))
    wide, tall = jax.ShapeDtypeStruct((dim, ff), BF16), jax.ShapeDtypeStruct((ff, dim), BF16)
    return pl.pallas_call(
        finish_kernel,
        grid_spec=pltpu.PrefetchScalarGridSpec(
            num_scalar_prefetch=1, grid=(ff // SLICE,), in_specs=[near, corner, near, corner],
            out_specs=[pl.BlockSpec(out.shape, lambda e, ids: (0, 0)) for out in (wide, wide, tall)]),
        out_shape=[wide, wide, tall], compiler_params=params(1), name="finish",
        cost_estimate=pl.CostEstimate(flops=1_000_000_000, bytes_accessed=16 * height * dim * 2, transcendentals=0),
    )(ids, *slices)


def solution(mesh):
    ep_size, tp_size = mesh.shape["ep"], mesh.shape["tp"]
    row_spec = P(("ep", "tp"), None)
    expert_spec = P("ep", None, None)
    expert_grad_spec = P("ep", "tp", None)
    swap = [(0, 1), (1, 0)]
    cores, along_x, along_y = ([(i, i ^ bit) for i in range(ep_size)] for bit in (1, 2, 4))

    def move(value, axis, route):
        return lax.ppermute(value, axis, route)

    def device_fn(tokens, grad_y, expert_ids, gate_vals, slot_ids,
                  shared_w1, shared_w3, shared_w2, expert_w1, expert_w3, expert_w2):
        rows_dev, dim = tokens.shape
        top_k = expert_ids.shape[1]
        local = expert_w1.shape[0]
        experts = local * ep_size
        cap = (2 * rows_dev * top_k + experts - 1) // experts
        tp_id, ep_id = lax.axis_index("tp"), lax.axis_index("ep")
        ids = jnp.stack([tp_id, ep_id]).astype(jnp.int32)

        pos = jnp.where(slot_ids >= 0, expert_ids * cap + slot_ids, -1).astype(F32)
        meta = jnp.concatenate([pos.T, gate_vals.T], axis=0)
        near_x, near_y, *others, far_own, far_other, meta_all, late_dy = gather_layer(tokens, grad_y, meta, ep_size)
        blocks = (tokens[None], near_x, near_y, *others)
        dy_all = lax.all_gather(late_dy, "ep")
        far_dy_all = lax.all_gather(move(late_dy, "tp", swap), "ep")
        far_meta = move(meta_all, "tp", swap)
        far_x, far_y = move(near_x, "tp", swap), move(near_y, "tp", swap)
        far_blocks = (far_own, far_x, far_y, far_other, move(far_x, "ep", cores), move(far_y, "ep", cores))

        ff = shared_w1.shape[1]
        padded = ep_size * SLICE
        wide_pad = ((0, 0), (0, padded - ff))
        start = ep_id * SLICE
        w1s = lax.dynamic_slice(jnp.pad(shared_w1, wide_pad), (0, start), (dim, SLICE))
        w3s = lax.dynamic_slice(jnp.pad(shared_w3, wide_pad), (0, start), (dim, SLICE))
        w2s = lax.dynamic_slice(jnp.pad(shared_w2, ((0, padded - ff), (0, 0))), (start, 0), (SLICE, dim))
        wa_own = jnp.concatenate([w1s, w3s], axis=1)
        wide = (wa_own, move(wa_own, "tp", swap))
        tall = (w2s, move(w2s, "tp", swap))

        sizes = (local, cap, top_k)
        xd, rows_select, rows_gate = dispatch_x(ids, blocks, meta_all, *sizes)
        o, h, a1, a3 = forward(xd, expert_w1, expert_w3, expert_w2, cap)
        qd = dispatch_dy(ids, dy_all, rows_select, rows_gate, local, cap)
        sh, sda, shared_grad, shared_far = shared_expert(ids, blocks, dy_all, wide + tall)
        y_part, select = combine_out(ids, meta_all, o, sh, tall, top_k)
        y_sum = lax.psum_scatter(y_part.reshape(-1, dim), "ep", scatter_dimension=0, tiled=True)
        dr, da1, da3 = backward(qd, a1, a3, expert_w1, expert_w3, expert_w2, cap)
        dx_part = combine_back(ids, select, dr, sda, wide)
        dx_sum = lax.psum_scatter(dx_part.reshape(-1, dim), "ep", scatter_dimension=0, tiled=True)

        xp, qp = dispatch_far(ids, far_blocks, far_dy_all, far_meta, *sizes)
        g1, g3, g2 = expert_grads(ids, xd, qd, xp, qp, h, da1, da3, expert_w1, expert_w3, expert_w2, tp_size)

        shared_grad = shared_grad + move(shared_far, "tp", swap)
        mine = shared_grad.astype(BF16)
        from_x, from_y = move(mine, "ep", along_x), move(mine, "ep", along_y)
        chips = jnp.stack([mine, from_x, from_y])
        corner = move(from_x, "ep", along_y)
        slices = (chips, corner[None], move(chips, "ep", cores), move(corner, "ep", cores)[None])
        sg1, sg3, sg2 = finish(ids, slices, ff)
        out_y = (tokens.astype(F32) + y_sum).astype(BF16)
        grad_tokens = (grad_y.astype(F32) + dx_sum).astype(BF16)
        return out_y, grad_tokens, sg1, sg3, sg2, g1, g3, g2

    return jax.shard_map(
        device_fn, mesh=mesh,
        in_specs=(row_spec, row_spec, row_spec, row_spec, row_spec,
                  P(None, "tp"), P(None, "tp"), P("tp", None), expert_spec, expert_spec, expert_spec),
        out_specs=(row_spec, row_spec, P(None, "tp"), P(None, "tp"), P("tp", None),
                   expert_grad_spec, expert_grad_spec, expert_grad_spec),
        check_vma=False)
```

```python
import functools

import jax
import jax.numpy as jnp
from jax import lax
from jax.experimental import pallas as pl
from jax.experimental.pallas import tpu as pltpu
from jax.sharding import PartitionSpec as P


F32 = jnp.float32
BF16 = jnp.bfloat16
SLICE = 128
VMEM_LIMIT = 64_000_000
MESH = pl.DeviceIdType.MESH
NT = (((1,), (1,)), ((), ()))
TN = (((0,), (0,)), ((), ()))


def dot(a, b):
    return jnp.dot(a, b, preferred_element_type=F32)


def dot_nt(a, b):
    return lax.dot_general(a, b, NT, preferred_element_type=F32)


def dot_tn(a, b):
    return lax.dot_general(a, b, TN, preferred_element_type=F32)


def swiglu_parts(one, three, grad_hidden):
    sig = jax.nn.sigmoid(one)
    silu = one * sig
    dh = grad_hidden.astype(BF16).astype(F32)
    hidden = (silu * three).astype(BF16)
    da_one = (dh * three * (sig + silu * (1.0 - sig))).astype(BF16)
    da_three = (dh * silu).astype(BF16)
    return hidden, da_one, da_three


def params(axes):
    return pltpu.CompilerParams(dimension_semantics=("arbitrary",) * axes, vmem_limit_bytes=VMEM_LIMIT)


def gather_kernel(ep_size, x_ref, dy_ref, meta_ref, near_x_ref, near_y_ref, other_own_ref, other_x_ref, other_y_ref,
                  far_own_ref, far_other_ref, meta_all_ref, dy_out_ref, mine, mine_dy, mine_meta,
                  load_sem, store_sem, send_sem, recv_sem):
    me = lax.axis_index("ep")
    core_peer = me + 1 - 2 * (me % 2)
    x_peer = me + 2 - 4 * ((me // 2) % 2)
    y_peer = me + 4 - 8 * (me // 4)
    z_peer = 1 - lax.axis_index("tp")

    barrier = pltpu.get_barrier_semaphore()
    for k in range(1, ep_size):
        pl.semaphore_signal(barrier, inc=1, device_id={"ep": (me + k) % ep_size}, device_id_type=MESH)
    pl.semaphore_signal(barrier, inc=1, device_id={"tp": z_peer}, device_id_type=MESH)

    loads = [pltpu.make_async_copy(x_ref, mine, load_sem.at[0]),
             pltpu.make_async_copy(meta_ref, mine_meta, load_sem.at[1]),
             pltpu.make_async_copy(dy_ref, mine_dy, load_sem.at[2])]
    for copy in loads:
        copy.start()
    for copy in loads:
        copy.wait()
    stores = [pltpu.make_async_copy(mine_dy, dy_out_ref, store_sem.at[0]),
              pltpu.make_async_copy(mine_meta, meta_all_ref.at[me], store_sem.at[1])]
    pl.semaphore_wait(barrier, ep_size)

    half = x_ref.shape[0] // 2
    low, high = pl.ds(0, half), pl.ds(half, half)
    started = []

    def send(device, src, dst):
        n = len(started)
        copy = pltpu.make_async_remote_copy(src_ref=src, dst_ref=dst, send_sem=send_sem.at[n], recv_sem=recv_sem.at[n],
                                            device_id=device, device_id_type=MESH)
        copy.start()
        started.append(copy)
        return copy

    to_x, to_y, to_core = {"ep": x_peer}, {"ep": y_peer}, {"ep": core_peer}
    from_x_low = send(to_x, mine.at[low], near_x_ref.at[0, low])
    from_y_high = send(to_y, mine.at[high], near_y_ref.at[0, high])
    from_z = send({"tp": z_peer}, mine, far_own_ref.at[0])
    from_x_high = send(to_x, mine.at[high], near_x_ref.at[0, high])
    from_y_low = send(to_y, mine.at[low], near_y_ref.at[0, low])
    waiting = [send({"ep": (me + k) % ep_size}, mine_meta, meta_all_ref.at[me]) for k in range(1, ep_size)]
    waiting.append(send(to_core, mine, other_own_ref.at[0]))
    for copy in stores:
        copy.start()
    from_x_low.wait_recv()
    corner_low = send(to_y, near_x_ref.at[0, low], near_y_ref.at[1, low])
    waiting.append(send(to_core, near_x_ref.at[0, low], other_x_ref.at[0, low]))
    from_y_high.wait_recv()
    corner_high = send(to_x, near_y_ref.at[0, high], near_y_ref.at[1, high])
    waiting.append(send(to_core, near_y_ref.at[0, high], other_y_ref.at[0, high]))
    from_x_high.wait_recv()
    waiting.append(send(to_core, near_x_ref.at[0, high], other_x_ref.at[0, high]))
    from_y_low.wait_recv()
    waiting.append(send(to_core, near_y_ref.at[0, low], other_y_ref.at[0, low]))
    from_z.wait_recv()
    waiting.append(send(to_core, far_own_ref.at[0], far_other_ref.at[0]))
    corner_low.wait_recv()
    waiting.append(send(to_core, near_y_ref.at[1, low], other_y_ref.at[1, low]))
    corner_high.wait_recv()
    waiting.append(send(to_core, near_y_ref.at[1, high], other_y_ref.at[1, high]))
    for copy in waiting:
        copy.wait_recv()
    for copy in started:
        copy.wait_send()
    for copy in stores:
        copy.wait()


def gather_layer(tokens, grad_y, meta, ep_size):
    rows, dim = tokens.shape
    one = jax.ShapeDtypeStruct((1, rows, dim), tokens.dtype)
    two = jax.ShapeDtypeStruct((2, rows, dim), tokens.dtype)
    anywhere = pl.BlockSpec(memory_space=pl.ANY)
    copies = 5 + (ep_size - 1) + 1 + 2 + 7
    return pl.pallas_call(
        functools.partial(gather_kernel, ep_size),
        in_specs=[anywhere] * 3, out_specs=[anywhere] * 9,
        out_shape=[one, two, one, one, two, one, one, jax.ShapeDtypeStruct((ep_size,) + meta.shape, meta.dtype),
                   jax.ShapeDtypeStruct(grad_y.shape, grad_y.dtype)],
        scratch_shapes=[pltpu.VMEM((rows, dim), tokens.dtype), pltpu.VMEM((rows, dim), grad_y.dtype),
                        pltpu.VMEM(meta.shape, meta.dtype), pltpu.SemaphoreType.DMA((3,)), pltpu.SemaphoreType.DMA((2,)),
                        pltpu.SemaphoreType.DMA((copies,)), pltpu.SemaphoreType.DMA((copies,))],
        compiler_params=pltpu.CompilerParams(collective_id=0, has_side_effects=True), name="gather",
        cost_estimate=pl.CostEstimate(flops=30_000_000_000, bytes_accessed=ep_size * rows * dim * 8, transcendentals=0),
    )(tokens, grad_y, meta)


def ep_of(source, ids):
    core = jnp.where(source < 4, ids[1] % 2, 1 - ids[1] % 2)
    return 2 * jnp.bitwise_xor(ids[1] // 2, source % 4) + core


def stream(refs, per_step, buffer, sem):
    blocks = [(ref, i) for ref in refs for i in range(ref.shape[0])]
    step = pl.program_id(0)
    steps = len(blocks) // per_step

    def copies(k):
        return [pltpu.make_async_copy(ref.at[i], buffer.at[k % 2, n], sem.at[k % 2, n])
                for n, (ref, i) in enumerate(blocks[k * per_step:(k + 1) * per_step])]

    @pl.when(step == 0)
    def _():
        for copy in copies(0):
            copy.start()

    for k in range(steps):
        @pl.when(step == k)
        def _():
            if k + 1 < steps:
                for copy in copies(k + 1):
                    copy.start()
            for copy in copies(k):
                copy.wait()

    return step % 2


def lay_rows(first, count, cap, got, out_ref):
    for l in range(count):
        out_ref[first + l] = got[l * cap:(l + 1) * cap].astype(BF16)


def gate_rows(meta, ids, total, first, rows, top_k):
    tokens = meta.shape[1]
    base = (ids[1] * total + first).astype(F32)
    row_ids = lax.broadcasted_iota(jnp.int32, (rows, tokens), 0).astype(F32) + base
    gates = jnp.zeros((rows, tokens), F32)
    for j in range(top_k):
        gates = jnp.where(meta[j][None, :] == row_ids, meta[top_k + j][None, :], gates)
    return gates, jnp.where(gates != 0.0, 1.0, 0.0).astype(BF16)


def dispatch_x_kernel(local, cap, top_k, ids, *refs):
    *blocks, meta_ref, xd_ref, select_ref, gate_ref, buffer, sem = refs
    slot = stream(blocks, 1, buffer, sem)
    meta = meta_ref[0]
    count = local // 2
    rows = count * cap
    for first in range(0, local, count):
        gates, select = gate_rows(meta, ids, local * cap, first * cap, rows, top_k)
        span = slice(first * cap, first * cap + rows)
        select_ref[0, span] = select
        gate_ref[0, span] = jnp.broadcast_to(jnp.sum(gates, axis=1, keepdims=True), (rows, gate_ref.shape[2]))
        lay_rows(first, count, cap, dot(select, buffer[slot, 0]), xd_ref)


def dispatch_x(ids, blocks, meta_all, local, cap, top_k):
    tokens, dim = blocks[0].shape[-2:]
    groups = sum(block.shape[0] for block in blocks)
    rows = local * cap
    return pl.pallas_call(
        functools.partial(dispatch_x_kernel, local, cap, top_k),
        grid_spec=pltpu.PrefetchScalarGridSpec(
            num_scalar_prefetch=1, grid=(groups,),
            in_specs=[pl.BlockSpec(memory_space=pl.ANY)] * len(blocks)
            + [pl.BlockSpec((1, 2 * top_k, tokens), lambda s, ids: (ep_of(s, ids), 0, 0))],
            out_specs=[pl.BlockSpec((local, cap, dim), lambda s, ids: (0, s, 0)),
                       pl.BlockSpec((1, rows, tokens), lambda s, ids: (s, 0, 0)),
                       pl.BlockSpec((1, rows, 128), lambda s, ids: (s, 0, 0))],
            scratch_shapes=[pltpu.VMEM((2, 1, tokens, dim), BF16), pltpu.SemaphoreType.DMA((2, 1))]),
        out_shape=[jax.ShapeDtypeStruct((local, groups * cap, dim), BF16),
                   jax.ShapeDtypeStruct((groups, rows, tokens), BF16), jax.ShapeDtypeStruct((groups, rows, 128), F32)],
        compiler_params=params(1), name="dispatch_x",
        cost_estimate=pl.CostEstimate(flops=2 * groups * rows * tokens * dim,
                                      bytes_accessed=groups * (tokens + rows) * dim * 2, transcendentals=0),
    )(ids, *blocks, meta_all)


def dispatch_dy_kernel(local, cap, ids, dy_ref, select_ref, gate_ref, qd_ref):
    lay_rows(0, local, cap, dot(select_ref[0], dy_ref[0]) * gate_ref[0][:, :1], qd_ref)


def dispatch_dy(ids, dy_all, select, gate, local, cap):
    groups, tokens, dim = dy_all.shape
    rows = local * cap
    by_place = lambda s, ids: (s, 0, 0)
    return pl.pallas_call(
        functools.partial(dispatch_dy_kernel, local, cap),
        grid_spec=pltpu.PrefetchScalarGridSpec(
            num_scalar_prefetch=1, grid=(groups,),
            in_specs=[pl.BlockSpec((1, tokens, dim), lambda s, ids: (ep_of(s, ids), 0, 0)),
                      pl.BlockSpec((1, rows, tokens), by_place), pl.BlockSpec((1, rows, 128), by_place)],
            out_specs=pl.BlockSpec((local, cap, dim), lambda s, ids: (0, s, 0))),
        out_shape=jax.ShapeDtypeStruct((local, groups * cap, dim), BF16), compiler_params=params(1), name="dispatch_dy",
        cost_estimate=pl.CostEstimate(flops=2 * groups * rows * tokens * dim,
                                      bytes_accessed=groups * (tokens + rows) * dim * 2, transcendentals=0),
    )(ids, dy_all, select, gate)


def dispatch_far_kernel(local, cap, top_k, ids, *refs):
    *blocks, dy_ref, meta_ref, xd_ref, qd_ref, buffer, sem = refs
    slot = stream(blocks, 1, buffer, sem)
    meta = meta_ref[0]
    count = local // 2
    for first in range(0, local, count):
        gates, select = gate_rows(meta, ids, local * cap, first * cap, count * cap, top_k)
        lay_rows(first, count, cap, dot(select, buffer[slot, 0]), xd_ref)
        lay_rows(first, count, cap, dot(select, dy_ref[0]) * jnp.sum(gates, axis=1, keepdims=True), qd_ref)


def dispatch_far(ids, blocks, dy_all, meta_all, local, cap, top_k):
    groups, tokens, dim = dy_all.shape
    by_ep = lambda s, ids: (ep_of(s, ids), 0, 0)
    out = jax.ShapeDtypeStruct((local, groups * cap, dim), BF16)
    out_spec = pl.BlockSpec((local, cap, dim), lambda s, ids: (0, s, 0))
    return pl.pallas_call(
        functools.partial(dispatch_far_kernel, local, cap, top_k),
        grid_spec=pltpu.PrefetchScalarGridSpec(
            num_scalar_prefetch=1, grid=(groups,),
            in_specs=[pl.BlockSpec(memory_space=pl.ANY)] * len(blocks)
            + [pl.BlockSpec((1, tokens, dim), by_ep), pl.BlockSpec((1, 2 * top_k, tokens), by_ep)],
            out_specs=[out_spec, out_spec],
            scratch_shapes=[pltpu.VMEM((2, 1, tokens, dim), BF16), pltpu.SemaphoreType.DMA((2, 1))]),
        out_shape=[out, out], compiler_params=params(1), name="dispatch_far",
        cost_estimate=pl.CostEstimate(flops=4 * groups * local * cap * tokens * dim,
                                      bytes_accessed=groups * (tokens + local * cap) * dim * 4, transcendentals=0),
    )(ids, *blocks, dy_all, meta_all)


def forward_kernel(cap, x_ref, w1_ref, w3_ref, w2_ref, o_ref, h_ref, a1_ref, a3_ref):
    rows = x_ref.shape[-2]
    half = rows // 2
    per = half // cap
    for part in range(2):
        span = slice(part * half, (part + 1) * half)
        x = x_ref[0, span]
        one, three = dot(x, w1_ref[0]), dot(x, w3_ref[0])
        hidden = (one * jax.nn.sigmoid(one) * three).astype(BF16)
        h_ref[0, span] = hidden
        a1_ref[0, span] = one
        a3_ref[0, span] = three
        out = dot(hidden, w2_ref[0])
        for s in range(per):
            o_ref[part * per + s] = out[s * cap:(s + 1) * cap].astype(BF16)


def forward(xd, w1, w3, w2, cap):
    local, rows, dim = xd.shape
    ff = w1.shape[-1]
    groups = rows // cap
    by_expert = lambda l: (l, 0, 0)
    hid_spec = pl.BlockSpec((1, rows, ff), by_expert)
    wide, tall = pl.BlockSpec((1, dim, ff), by_expert), pl.BlockSpec((1, ff, dim), by_expert)
    proj = jax.ShapeDtypeStruct((local, rows, ff), F32)
    return pl.pallas_call(
        functools.partial(forward_kernel, cap), grid=(local,),
        in_specs=[pl.BlockSpec((1, rows, dim), by_expert), wide, wide, tall],
        out_specs=[pl.BlockSpec((groups, cap, dim), lambda l: (0, l, 0)), hid_spec, hid_spec, hid_spec],
        out_shape=[jax.ShapeDtypeStruct((groups, local * cap, dim), BF16), jax.ShapeDtypeStruct((local, rows, ff), BF16),
                   proj, proj],
        compiler_params=params(1), name="forward",
        cost_estimate=pl.CostEstimate(flops=6 * local * rows * dim * ff,
                                      bytes_accessed=local * (4 * rows * dim + 10 * rows * ff + 6 * dim * ff),
                                      transcendentals=local * rows * ff),
    )(xd, w1, w3, w2)


def backward_kernel(cap, q_ref, a1_ref, a3_ref, w1_ref, w3_ref, w2_ref, dr_ref, da1_ref, da3_ref):
    rows = q_ref.shape[-2]
    half = rows // 2
    per = half // cap
    for part in range(2):
        span = slice(part * half, (part + 1) * half)
        _, da_one, da_three = swiglu_parts(a1_ref[0, span], a3_ref[0, span], dot_nt(q_ref[0, span], w2_ref[0]))
        da1_ref[0, span] = da_one
        da3_ref[0, span] = da_three
        grad = dot_nt(da_one, w1_ref[0]) + dot_nt(da_three, w3_ref[0])
        for s in range(per):
            dr_ref[part * per + s] = grad[s * cap:(s + 1) * cap].astype(BF16)


def backward(qd, a1, a3, w1, w3, w2, cap):
    local, rows, dim = qd.shape
    ff = w1.shape[-1]
    groups = rows // cap
    by_expert = lambda l: (l, 0, 0)
    hid_spec = pl.BlockSpec((1, rows, ff), by_expert)
    wide, tall = pl.BlockSpec((1, dim, ff), by_expert), pl.BlockSpec((1, ff, dim), by_expert)
    hid = jax.ShapeDtypeStruct((local, rows, ff), BF16)
    return pl.pallas_call(
        functools.partial(backward_kernel, cap), grid=(local,),
        in_specs=[pl.BlockSpec((1, rows, dim), by_expert), hid_spec, hid_spec, wide, wide, tall],
        out_specs=[pl.BlockSpec((groups, cap, dim), lambda l: (0, l, 0)), hid_spec, hid_spec],
        out_shape=[jax.ShapeDtypeStruct((groups, local * cap, dim), BF16), hid, hid],
        compiler_params=params(1), name="backward",
        cost_estimate=pl.CostEstimate(flops=6 * local * rows * dim * ff,
                                      bytes_accessed=local * (4 * rows * dim + 12 * rows * ff + 6 * dim * ff),
                                      transcendentals=local * rows * ff),
    )(qd, a1, a3, w1, w3, w2)


def grads_kernel(ids, x_ref, q_ref, xp_ref, qp_ref, h_ref, da1_ref, da3_ref, w1_ref, w3_ref, w2_ref,
                 g1_ref, g3_ref, g2_ref, rows_x, rows_q, hid, da_one, da_three, tall):
    rows = x_ref.shape[-2]
    half = rows // 2
    part = ids[0]
    width = g1_ref.shape[1]
    columns = pl.ds(pl.multiple_of(part * width, 128), width)
    ff = w1_ref.shape[-1]
    reach = tall.shape[0]
    chunk = pl.ds(pl.multiple_of(part * (ff - reach), 128), reach)
    rows_x[:rows] = x_ref[0, :, columns]
    rows_x[rows:] = xp_ref[0, :, columns]
    rows_q[:rows] = q_ref[0]
    rows_q[rows:] = qp_ref[0]
    hid[:rows] = h_ref[0]
    da_one[:rows] = da1_ref[0]
    da_three[:rows] = da3_ref[0]
    for piece in range(2):
        span = slice(piece * half, (piece + 1) * half)
        dest = slice(rows + piece * half, rows + (piece + 1) * half)
        x = xp_ref[0, span]
        hidden, one, three = swiglu_parts(dot(x, w1_ref[0]), dot(x, w3_ref[0]), dot_nt(qp_ref[0, span], w2_ref[0]))
        hid[dest] = hidden
        da_one[dest] = one
        da_three[dest] = three
    g1_ref[0] = dot_tn(rows_x[...], da_one[...]).astype(BF16)
    g3_ref[0] = dot_tn(rows_x[...], da_three[...]).astype(BF16)
    height = g2_ref.shape[1]
    tall[...] = dot_tn(hid[:, chunk], rows_q[...])
    skip = pl.multiple_of(part * (height - (ff - reach)), 8)
    g2_ref[0] = tall[pl.ds(skip, height)].astype(BF16)


def expert_grads(ids, xd, qd, xp, qp, h, da1, da3, w1, w3, w2, parts):
    local, rows, dim = xd.shape
    ff = w1.shape[-1]
    by_expert = lambda l, ids: (l, 0, 0)
    row_spec, hid_spec = pl.BlockSpec((1, rows, dim), by_expert), pl.BlockSpec((1, rows, ff), by_expert)
    wide, tall = pl.BlockSpec((1, dim, ff), by_expert), pl.BlockSpec((1, ff, dim), by_expert)
    g1 = jax.ShapeDtypeStruct((local, dim // parts, ff), BF16)
    g2 = jax.ShapeDtypeStruct((local, ff // parts, dim), BF16)
    g1_spec, g2_spec = pl.BlockSpec((1, dim // parts, ff), by_expert), pl.BlockSpec((1, ff // parts, dim), by_expert)
    reach = -(-(ff // parts) // 128) * 128
    return pl.pallas_call(
        grads_kernel,
        grid_spec=pltpu.PrefetchScalarGridSpec(
            num_scalar_prefetch=1, grid=(local,),
            in_specs=[row_spec, row_spec, row_spec, row_spec, hid_spec, hid_spec, hid_spec, wide, wide, tall],
            out_specs=[g1_spec, g1_spec, g2_spec],
            scratch_shapes=[pltpu.VMEM((2 * rows, dim // parts), BF16), pltpu.VMEM((2 * rows, dim), BF16)]
            + [pltpu.VMEM((2 * rows, ff), BF16)] * 3 + [pltpu.VMEM((reach, dim), F32)]),
        out_shape=[g1, g1, g2], compiler_params=params(1), name="grads",
        cost_estimate=pl.CostEstimate(flops=12 * local * rows * dim * ff,
                                      bytes_accessed=local * (8 * rows * dim + 6 * rows * ff + 9 * dim * ff),
                                      transcendentals=local * rows * ff),
    )(ids, xd, qd, xp, qp, h, da1, da3, w1, w3, w2)


def shared_kernel(ids, *refs):
    *blocks, dy_one_ref, dy_two_ref, wa_ref, wa_far_ref, w2_ref, w2_far_ref, h_ref, da_ref, g_ref, g_far_ref, buffer, sem = refs
    slot = stream(blocks, 2, buffer, sem)

    @pl.when(pl.program_id(0) == 0)
    def _():
        g_ref[...] = jnp.zeros_like(g_ref)
        g_far_ref[...] = jnp.zeros_like(g_far_ref)

    _, pair, tokens, dim = buffer.shape
    x = buffer[slot].reshape(pair * tokens, dim)
    dy = jnp.concatenate([dy_one_ref[0], dy_two_ref[0]], axis=0)
    for half, (grad_ref, up_ref, down_ref) in enumerate(((g_ref, wa_ref, w2_ref), (g_far_ref, wa_far_ref, w2_far_ref))):
        proj = dot(x, up_ref[...])
        hidden, da_one, da_three = swiglu_parts(proj[:, :SLICE], proj[:, SLICE:], dot_nt(dy, down_ref[...]))
        da = jnp.concatenate([da_one, da_three], axis=1)
        h_ref[:, :, half * SLICE:(half + 1) * SLICE] = hidden.reshape(pair, tokens, SLICE)
        da_ref[:, :, 2 * half * SLICE:2 * (half + 1) * SLICE] = da.reshape(pair, tokens, 2 * SLICE)
        grad_ref[:2 * SLICE] += dot_tn(da, x)
        grad_ref[2 * SLICE:] += dot_tn(hidden, dy)


def shared_expert(ids, blocks, dy_all, weights):
    groups, tokens, dim = dy_all.shape
    by_pair, fixed = lambda s, ids: (s, 0, 0), lambda s, ids: (0, 0)
    grad = jax.ShapeDtypeStruct((3 * SLICE, dim), F32)
    return pl.pallas_call(
        shared_kernel,
        grid_spec=pltpu.PrefetchScalarGridSpec(
            num_scalar_prefetch=1, grid=(groups // 2,),
            in_specs=[pl.BlockSpec(memory_space=pl.ANY)] * len(blocks)
            + [pl.BlockSpec((1, tokens, dim), lambda s, ids: (ep_of(2 * s, ids), 0, 0)),
               pl.BlockSpec((1, tokens, dim), lambda s, ids: (ep_of(2 * s + 1, ids), 0, 0)),
               ] + [pl.BlockSpec(weight.shape, fixed) for weight in weights],
            out_specs=[pl.BlockSpec((2, tokens, 2 * SLICE), by_pair), pl.BlockSpec((2, tokens, 4 * SLICE), by_pair),
                       pl.BlockSpec(grad.shape, fixed), pl.BlockSpec(grad.shape, fixed)],
            scratch_shapes=[pltpu.VMEM((2, 2, tokens, dim), BF16), pltpu.SemaphoreType.DMA((2, 2))]),
        out_shape=[jax.ShapeDtypeStruct((groups, tokens, 2 * SLICE), BF16),
                   jax.ShapeDtypeStruct((groups, tokens, 4 * SLICE), BF16), grad, grad],
        compiler_params=params(1), name="shared",
        cost_estimate=pl.CostEstimate(flops=18 * groups * tokens * dim * SLICE,
                                      bytes_accessed=4 * groups * tokens * dim, transcendentals=0),
    )(ids, *blocks, dy_all, dy_all, *weights)


def gate_matrix(meta, ids, rows, top_k):
    tokens = meta.shape[0]
    base = (ids[1] * rows).astype(F32)
    row_ids = lax.broadcasted_iota(jnp.int32, (tokens, rows), 1).astype(F32) + base
    gates = jnp.zeros((tokens, rows), F32)
    for j in range(top_k):
        gates = jnp.where(meta[:, j:j + 1] == row_ids, meta[:, top_k + j:top_k + j + 1], gates)
    return gates


def combine_out_kernel(top_k, ids, meta_ref, o_ref, h_ref, w2_ref, w2_far_ref, y_ref, select_ref):
    tokens = h_ref.shape[1]
    meta = meta_ref[0].T
    width = w2_ref.shape[0]
    part = tokens // 2
    for first in range(0, tokens, part):
        span = slice(first, first + part)
        gates = gate_matrix(meta[span], ids, o_ref.shape[1], top_k)
        select_ref[0, span] = jnp.where(gates != 0.0, 1.0, 0.0).astype(BF16)
        high = gates.astype(BF16)
        rest = gates - high.astype(F32)
        mid = rest.astype(BF16)
        low = (rest - mid.astype(F32)).astype(BF16)
        sums = dot(jnp.concatenate([high, mid, low], axis=0), o_ref[0])
        y_ref[0, span] = (sums[:part] + sums[part:2 * part] + sums[2 * part:]
                          + dot(h_ref[0, span, :width], w2_ref[...]) + dot(h_ref[0, span, width:], w2_far_ref[...]))


def combine_out(ids, meta_all, o, h, weights, top_k):
    groups, rows, dim = o.shape
    tokens, width = h.shape[1:]
    by_place = lambda s, ids: (s, 0, 0)
    by_ep = lambda s, ids: (ep_of(s, ids), 0, 0)
    return pl.pallas_call(
        functools.partial(combine_out_kernel, top_k),
        grid_spec=pltpu.PrefetchScalarGridSpec(
            num_scalar_prefetch=1, grid=(groups,),
            in_specs=[pl.BlockSpec((1, 2 * top_k, tokens), by_ep), pl.BlockSpec((1, rows, dim), by_place),
                      pl.BlockSpec((1, tokens, width), by_place)]
            + [pl.BlockSpec(weight.shape, lambda s, ids: (0, 0)) for weight in weights],
            out_specs=[pl.BlockSpec((1, tokens, dim), by_ep), pl.BlockSpec((1, tokens, rows), by_place)]),
        out_shape=[jax.ShapeDtypeStruct((groups, tokens, dim), F32), jax.ShapeDtypeStruct((groups, tokens, rows), BF16)],
        compiler_params=params(1), name="combine_out",
        cost_estimate=pl.CostEstimate(flops=6 * groups * tokens * rows * dim,
                                      bytes_accessed=groups * (2 * rows + 4 * tokens) * dim, transcendentals=0),
    )(ids, meta_all, o, h, *weights)


def combine_back_kernel(ids, select_ref, dr_ref, da_ref, wa_ref, wa_far_ref, dx_ref):
    width = wa_ref.shape[1]
    dx_ref[0] = (dot(select_ref[0], dr_ref[0]) + dot_nt(da_ref[0, :, :width], wa_ref[...])
                 + dot_nt(da_ref[0, :, width:], wa_far_ref[...]))


def combine_back(ids, select, dr, da, weights):
    groups, rows, dim = dr.shape
    tokens, width = da.shape[1:]
    by_place = lambda s, ids: (s, 0, 0)
    return pl.pallas_call(
        combine_back_kernel,
        grid_spec=pltpu.PrefetchScalarGridSpec(
            num_scalar_prefetch=1, grid=(groups,),
            in_specs=[pl.BlockSpec((1, tokens, rows), by_place), pl.BlockSpec((1, rows, dim), by_place),
                      pl.BlockSpec((1, tokens, width), by_place)]
            + [pl.BlockSpec(weight.shape, lambda s, ids: (0, 0)) for weight in weights],
            out_specs=pl.BlockSpec((1, tokens, dim), lambda s, ids: (ep_of(s, ids), 0, 0))),
        out_shape=jax.ShapeDtypeStruct((groups, tokens, dim), F32), compiler_params=params(1), name="combine_back",
        cost_estimate=pl.CostEstimate(flops=2 * groups * tokens * (rows + width) * dim,
                                      bytes_accessed=groups * (2 * rows + 4 * tokens) * dim, transcendentals=0),
    )(ids, select, dr, da, *weights)


def finish_kernel(ids, near_ref, corner_ref, other_near_ref, other_corner_ref, g1_ref, g3_ref, g2_ref):
    device = pl.program_id(0)
    place = pl.ds(pl.multiple_of(device * SLICE, SLICE), SLICE)

    def lay(ref):
        g1_ref[:, place] = ref[0, :SLICE].T
        g3_ref[:, place] = ref[0, SLICE:2 * SLICE].T
        g2_ref[place] = ref[0, 2 * SLICE:]

    same = device % 2 == ids[1] % 2
    near = jnp.bitwise_xor(device // 2, ids[1] // 2) < 3
    pl.when(same & near)(lambda: lay(near_ref))
    pl.when(same & jnp.logical_not(near))(lambda: lay(corner_ref))
    pl.when(jnp.logical_not(same) & near)(lambda: lay(other_near_ref))
    pl.when(jnp.logical_not(same) & jnp.logical_not(near))(lambda: lay(other_corner_ref))


def finish(ids, slices, ff):
    _, height, dim = slices[0].shape
    near = pl.BlockSpec((1, height, dim), lambda e, ids: (jnp.minimum(jnp.bitwise_xor(e // 2, ids[1] // 2), 2), 0, 0))
    corner = pl.BlockSpec((1, height, dim), lambda e, ids: (0, 0, 0))
    wide, tall = jax.ShapeDtypeStruct((dim, ff), BF16), jax.ShapeDtypeStruct((ff, dim), BF16)
    return pl.pallas_call(
        finish_kernel,
        grid_spec=pltpu.PrefetchScalarGridSpec(
            num_scalar_prefetch=1, grid=(ff // SLICE,), in_specs=[near, corner, near, corner],
            out_specs=[pl.BlockSpec(out.shape, lambda e, ids: (0, 0)) for out in (wide, wide, tall)]),
        out_shape=[wide, wide, tall], compiler_params=params(1), name="finish",
        cost_estimate=pl.CostEstimate(flops=1_000_000_000, bytes_accessed=16 * height * dim * 2, transcendentals=0),
    )(ids, *slices)


def solution(mesh):
    ep_size, tp_size = mesh.shape["ep"], mesh.shape["tp"]
    row_spec = P(("ep", "tp"), None)
    expert_spec = P("ep", None, None)
    expert_grad_spec = P("ep", "tp", None)
    swap = [(0, 1), (1, 0)]
    cores, along_x, along_y = ([(i, i ^ bit) for i in range(ep_size)] for bit in (1, 2, 4))

    def move(value, axis, route):
        return lax.ppermute(value, axis, route)

    def device_fn(tokens, grad_y, expert_ids, gate_vals, slot_ids,
                  shared_w1, shared_w3, shared_w2, expert_w1, expert_w3, expert_w2):
        rows_dev, dim = tokens.shape
        top_k = expert_ids.shape[1]
        local = expert_w1.shape[0]
        experts = local * ep_size
        cap = (2 * rows_dev * top_k + experts - 1) // experts
        tp_id, ep_id = lax.axis_index("tp"), lax.axis_index("ep")
        ids = jnp.stack([tp_id, ep_id]).astype(jnp.int32)

        pos = jnp.where(slot_ids >= 0, expert_ids * cap + slot_ids, -1).astype(F32)
        meta = jnp.concatenate([pos.T, gate_vals.T], axis=0)
        near_x, near_y, *others, far_own, far_other, meta_all, late_dy = gather_layer(tokens, grad_y, meta, ep_size)
        blocks = (tokens[None], near_x, near_y, *others)
        dy_all = lax.all_gather(late_dy, "ep")
        far_dy_all = lax.all_gather(move(late_dy, "tp", swap), "ep")
        far_meta = move(meta_all, "tp", swap)
        far_x, far_y = move(near_x, "tp", swap), move(near_y, "tp", swap)
        far_blocks = (far_own, far_x, far_y, far_other, move(far_x, "ep", cores), move(far_y, "ep", cores))

        ff = shared_w1.shape[1]
        padded = ep_size * SLICE
        wide_pad = ((0, 0), (0, padded - ff))
        start = ep_id * SLICE
        w1s = lax.dynamic_slice(jnp.pad(shared_w1, wide_pad), (0, start), (dim, SLICE))
        w3s = lax.dynamic_slice(jnp.pad(shared_w3, wide_pad), (0, start), (dim, SLICE))
        w2s = lax.dynamic_slice(jnp.pad(shared_w2, ((0, padded - ff), (0, 0))), (start, 0), (SLICE, dim))
        wa_own = jnp.concatenate([w1s, w3s], axis=1)
        wide = (wa_own, move(wa_own, "tp", swap))
        tall = (w2s, move(w2s, "tp", swap))

        sizes = (local, cap, top_k)
        xd, rows_select, rows_gate = dispatch_x(ids, blocks, meta_all, *sizes)
        o, h, a1, a3 = forward(xd, expert_w1, expert_w3, expert_w2, cap)
        qd = dispatch_dy(ids, dy_all, rows_select, rows_gate, local, cap)
        sh, sda, shared_grad, shared_far = shared_expert(ids, blocks, dy_all, wide + tall)
        y_part, select = combine_out(ids, meta_all, o, sh, tall, top_k)
        y_sum = lax.psum_scatter(y_part.reshape(-1, dim), "ep", scatter_dimension=0, tiled=True)
        dr, da1, da3 = backward(qd, a1, a3, expert_w1, expert_w3, expert_w2, cap)
        dx_part = combine_back(ids, select, dr, sda, wide)
        dx_sum = lax.psum_scatter(dx_part.reshape(-1, dim), "ep", scatter_dimension=0, tiled=True)

        xp, qp = dispatch_far(ids, far_blocks, far_dy_all, far_meta, *sizes)
        g1, g3, g2 = expert_grads(ids, xd, qd, xp, qp, h, da1, da3, expert_w1, expert_w3, expert_w2, tp_size)

        shared_grad = shared_grad + move(shared_far, "tp", swap)
        mine = shared_grad.astype(BF16)
        from_x, from_y = move(mine, "ep", along_x), move(mine, "ep", along_y)
        chips = jnp.stack([mine, from_x, from_y])
        corner = move(from_x, "ep", along_y)
        slices = (chips, corner[None], move(chips, "ep", cores), move(corner, "ep", cores)[None])
        sg1, sg3, sg2 = finish(ids, slices, ff)
        out_y = (tokens.astype(F32) + y_sum).astype(BF16)
        grad_tokens = (grad_y.astype(F32) + dx_sum).astype(BF16)
        return out_y, grad_tokens, sg1, sg3, sg2, g1, g3, g2

    return jax.shard_map(
        device_fn, mesh=mesh,
        in_specs=(row_spec, row_spec, row_spec, row_spec, row_spec,
                  P(None, "tp"), P(None, "tp"), P("tp", None), expert_spec, expert_spec, expert_spec),
        out_specs=(row_spec, row_spec, P(None, "tp"), P(None, "tp"), P("tp", None),
                   expert_grad_spec, expert_grad_spec, expert_grad_spec),
        check_vma=False)
```
